256 devices in a mesh: dp: 8 (over x, y_lo), ctx: 32 (over y_hi, z, core).
Axes of the slice: x: 4, y: 4 (y_hi: 2, y_lo: 2; y = y_hi * 2 + y_lo), z: 8, core: 2. Of those that a mesh axis runs over, the one named last changes fastest.
Arguments:
- query_matrix: bfloat16 [8, 4096, 2048], P('dp', 'ctx'), may hold values from -16 to 16
- key_matrix: bfloat16 [8, 4096, 512], P('dp', 'ctx'), may hold values from -16 to 16
- value_matrix: bfloat16 [8, 4096, 512], P('dp', 'ctx'), may hold values from -6 to 6
- output_gradient: bfloat16 [8, 4096, 2048], P('dp', 'ctx'), may hold values from -6 to 6
- hidden_in: bfloat16 [8, 4096, 4096], P('dp', 'ctx'), may hold values from -6 to 6
- doc_lengths: int32 [8, 16], P('dp'), may hold values from 1 to 3072, 4096 in all within a row
- querya: bfloat16 [16, 4096], replicated, may hold values from -0.09375 to 0.09375
- queryb: bfloat16 [16, 2048], replicated, may hold values from -1.5 to 1.5
- valuea: bfloat16 [16, 4096], replicated, may hold values from -0.09375 to 0.09375
- valueb: bfloat16 [16, 512], replicated, may hold values from -1.5 to 1.5
Outputs:
- query_grad: bfloat16 [8, 4096, 2048], P('dp', 'ctx')
- key_grad: bfloat16 [8, 4096, 512], P('dp', 'ctx')
- value_gradient: bfloat16 [8, 4096, 512], P('dp', 'ctx')
- querya_grad: float32 [16, 4096], replicated
- queryb_grad: float32 [16, 2048], replicated
- valuea_grad: float32 [16, 4096], replicated
- valueb_grad: float32 [16, 512], replicated
The draws below stay inside these ranges and needn't reach their ends.
Inputs may be any that keep to these rules, and one draw needn't show every extreme that they name: `doc_lengths`: row b lists, in order, the lengths of the 16 documents packed into sequence b; they sum to 4096.
All inputs are finite; a program needn't handle non-finite values.
Results may differ from the reference program's by a relative error of at most 0.022.
Values may be sent and summed in bfloat16 or wider, within the bound.
A program may use at most 128 MiB of HBM per device.

```python
import math
import jax
import jax.numpy as jnp
import numpy as np
from jax import lax

D = 4096
QUERY_HEADS = 16
KEY_VALUE_HEADS = 4
HEAD_WIDTH = 128
ADAPTER_RANK = 16
DOCS = 16
TOKENS_PER_SHARD = 128
SEQUENCE_LENGTH = 4096
BATCH_SEQUENCES = 8
N_CTX = 32


def paired_fields(key):
    base_key = jax.random.fold_in(key, 31)
    random_query, random_keys = jax.random.split(base_key, 2)
    group_width = QUERY_HEADS // KEY_VALUE_HEADS
    query_list = jnp.clip(jax.random.normal(random_query, (BATCH_SEQUENCES, SEQUENCE_LENGTH, KEY_VALUE_HEADS, group_width, HEAD_WIDTH), jnp.float32), -4.0, 4.0)
    key_collection = jnp.clip(jax.random.normal(random_keys, (BATCH_SEQUENCES, SEQUENCE_LENGTH, KEY_VALUE_HEADS, HEAD_WIDTH), jnp.float32), -3.0, 3.0)
    return (query_list.reshape(BATCH_SEQUENCES, SEQUENCE_LENGTH, QUERY_HEADS * HEAD_WIDTH), key_collection.reshape(BATCH_SEQUENCES, SEQUENCE_LENGTH, KEY_VALUE_HEADS * HEAD_WIDTH))


def draw_query_matrix(key, part):
    return paired_fields(key)[0].astype(jnp.bfloat16)


def draw_key_matrix(key, part):
    return paired_fields(key)[1].astype(jnp.bfloat16)


def steps_of(own_key, dims, shards, low, high):
    def one(dim, shards_of):
        draws = jax.random.uniform(jax.random.fold_in(jax.random.fold_in(own_key, 6), dim), (shards_of,), jnp.float32, low / len(shards), high / len(shards))
        return jnp.repeat(jnp.exp(draws), dims[dim] // shards_of).reshape((-1,) + (1,) * (len(dims) - dim - 1))

    factor_of = one(*shards[0])
    for cut in shards[1:]:
        factor_of = factor_of * one(*cut)
    return factor_of


def profile(number_of, total, reach, slope):
    loads = [(1 << 20) // math.isqrt(grade ** slope) + 1 for grade in range(2, number_of + 1)]
    surplus, given = total - reach - (number_of - 1), [1] * (number_of - 1)
    while surplus > 0:
        free = [i for i in range(number_of - 1) if given[i] < reach]
        whole, left = sum([loads[i] for i in free]), surplus
        for i in free:
            extra = min(reach - given[i], max(1, left * loads[i] // whole), surplus)
            given[i] = given[i] + extra
            surplus = surplus - extra
    return np.array([reach] + given)


def uneven_parts(stream_key, amount, total, limit, skew):
    if amount == 2:
        one = jax.random.randint(stream_key, (), max(1, total - limit), min(limit, total - 1) + 1)
        return jnp.stack([one, total - one])
    sizes = jnp.asarray(profile(amount, total, limit, skew), jnp.int32)
    pairs = (amount - 1) // 2
    source_of, taker = sizes[1:1 + 2 * pairs:2], sizes[2:2 + 2 * pairs:2]
    slack = jnp.minimum(source_of - 1, limit - taker)
    passed = jax.random.randint(jax.random.fold_in(stream_key, 1), (pairs,), 0, 1 << 20) % (slack + 1)
    sizes = sizes.at[1:1 + 2 * pairs:2].set(source_of - passed).at[2:2 + 2 * pairs:2].set(taker + passed)
    return sizes[jax.random.permutation(jax.random.fold_in(stream_key, 2), amount)]


def noise(rng, shape, deviation, most, cuts=(), held_as=jnp.bfloat16):
    values = deviation * jax.random.normal(rng, shape, jnp.float32)
    if cuts:
        values = values * steps_of(rng, shape, cuts, -0.22, 0.18)
    return jnp.clip(values, -most, most).astype(held_as)


def setup_inputs(seed: int = 0) -> dict:
    arg_keys = jax.random.split(jax.random.key(seed), 11)
    query_matrix = draw_query_matrix(jax.random.fold_in(arg_keys[10], 71), 0)
    key_matrix = draw_key_matrix(jax.random.fold_in(arg_keys[10], 71), 0)
    value_matrix = noise(arg_keys[2], (BATCH_SEQUENCES, SEQUENCE_LENGTH, KEY_VALUE_HEADS * HEAD_WIDTH), 1.0, 6.0, ((0, 8), (1, 32)))
    output_gradient = noise(arg_keys[3], (BATCH_SEQUENCES, SEQUENCE_LENGTH, QUERY_HEADS * HEAD_WIDTH), 1.0, 6.0, ((0, 8), (1, 32)))
    hidden_in = noise(arg_keys[4], (BATCH_SEQUENCES, SEQUENCE_LENGTH, D), 1.0, 6.0, ((0, 8), (1, 32)))
    doc_lengths = jax.vmap(lambda own: uneven_parts(own, DOCS, SEQUENCE_LENGTH, 3 * SEQUENCE_LENGTH // 4, 2))(jax.random.split(arg_keys[5], BATCH_SEQUENCES)).reshape((BATCH_SEQUENCES, DOCS)).astype(jnp.int32)
    querya = noise(arg_keys[6], (ADAPTER_RANK, D), D ** -0.5, 0.09375)
    queryb = noise(arg_keys[7], (ADAPTER_RANK, QUERY_HEADS * HEAD_WIDTH), ADAPTER_RANK ** -0.5, 1.5)
    valuea = noise(arg_keys[8], (ADAPTER_RANK, D), D ** -0.5, 0.09375)
    valueb = noise(arg_keys[9], (ADAPTER_RANK, KEY_VALUE_HEADS * HEAD_WIDTH), ADAPTER_RANK ** -0.5, 1.5)
    return dict(query_matrix=query_matrix, key_matrix=key_matrix, value_matrix=value_matrix, output_gradient=output_gradient, hidden_in=hidden_in, doc_lengths=doc_lengths, querya=querya, queryb=queryb, valuea=valuea, valueb=valueb)


NEG_FILL = -1.0e30
ADAPTER_SCALE = 2.0


def doc_begin(lengths, positions):
    doc_ends = jnp.cumsum(lengths).astype(jnp.int32)
    begins = (doc_ends - lengths).astype(jnp.int32)
    inside = begins[None, :] <= positions[:, None]
    return jnp.max(jnp.where(inside, begins[None, :], 0), axis=1).astype(jnp.int32)


def rounded_length(values):
    return lax.optimization_barrier(values.astype(jnp.bfloat16)).astype(jnp.float32)


def contract_last(left, right):
    return lax.dot_general(left, right, (((1,), (1,)), ((), ())), preferred_element_type=jnp.float32)


def contract_first(left, right):
    return lax.dot_general(left, right, (((0,), (0,)), ((), ())), preferred_element_type=jnp.float32)


def sequence_grads(packed):
    query_matrix, key_matrix, value_matrix, output_gradient, lengths = packed
    sequence_total = TOKENS_PER_SHARD * N_CTX
    group_width = QUERY_HEADS // KEY_VALUE_HEADS
    rows_per_half = TOKENS_PER_SHARD // 2
    head_scale = HEAD_WIDTH ** -0.5
    positions = lax.iota(jnp.int32, sequence_total)
    begins = doc_begin(lengths, positions)
    key_quad = key_matrix.reshape(sequence_total, KEY_VALUE_HEADS, HEAD_WIDTH).astype(jnp.float32)
    value_quad = value_matrix.reshape(sequence_total, KEY_VALUE_HEADS, HEAD_WIDTH).astype(jnp.float32)
    query_block_list = query_matrix.reshape(N_CTX, TOKENS_PER_SHARD, KEY_VALUE_HEADS, group_width, HEAD_WIDTH)
    gradient_block_list = output_gradient.reshape(N_CTX, TOKENS_PER_SHARD, KEY_VALUE_HEADS, group_width, HEAD_WIDTH)
    pos_blocks = positions.reshape(N_CTX, TOKENS_PER_SHARD)
    begin_blocks = begins.reshape(N_CTX, TOKENS_PER_SHARD)

    def one_block(carry_in, inputs):
        key_total_sum, value_total_sum = carry_in
        query_block, grad_block, pos_block, begin_block = inputs
        query_wide = query_block.astype(jnp.float32)
        gradient_wide = grad_block.astype(jnp.float32)
        visible = ((positions[None, :] <= pos_block[:, None]) & (positions[None, :] >= begin_block[:, None]))[:, None, None, :]
        scores = jnp.einsum("thgd,chd->thgc", query_wide, key_quad) * head_scale
        row_max = jnp.max(jnp.where(visible, scores, NEG_FILL), axis=-1)
        unnorm = jnp.where(visible, jnp.exp(scores - row_max[..., None]), 0.0)
        row_total = jnp.sum(unnorm, axis=-1)
        attended = jnp.einsum("thgc,chd->thgd", rounded_length(unnorm), value_quad) / row_total[..., None]
        log_total = row_max + jnp.log(row_total)
        delta_rows = jnp.sum(gradient_wide * attended, axis=-1)
        probabilities = jnp.where(visible, jnp.exp(scores - log_total[..., None]), 0.0)
        grad_probs = jnp.einsum("thgd,chd->thgc", gradient_wide, value_quad)
        score_gradient = rounded_length(probabilities * (grad_probs - delta_rows[..., None]) * head_scale)
        query_grad = jnp.einsum("thgc,chd->thgd", score_gradient, key_quad).astype(jnp.bfloat16)
        score_split_halves = score_gradient.reshape(2, rows_per_half, KEY_VALUE_HEADS, group_width, sequence_total)
        probability_halves = rounded_length(probabilities).reshape(2, rows_per_half, KEY_VALUE_HEADS, group_width, sequence_total)
        query_split_halves = query_wide.reshape(2, rows_per_half, KEY_VALUE_HEADS, group_width, HEAD_WIDTH)
        gradient_halves = gradient_wide.reshape(2, rows_per_half, KEY_VALUE_HEADS, group_width, HEAD_WIDTH)
        key_part = jnp.sum(rounded_length(jnp.einsum("pthgc,pthgd->pchd", score_split_halves, query_split_halves)), axis=0)
        value_part = jnp.sum(rounded_length(jnp.einsum("pthgc,pthgd->pchd", probability_halves, gradient_halves)), axis=0)
        return (key_total_sum + key_part, value_total_sum + value_part), query_grad

    zero_sum_start = jnp.zeros((sequence_total, KEY_VALUE_HEADS, HEAD_WIDTH), jnp.float32)
    (key_total_sum, value_total_sum), query_grads = lax.scan(one_block, (zero_sum_start, zero_sum_start), (query_block_list, gradient_block_list, pos_blocks, begin_blocks))
    return (query_grads.reshape(sequence_total, QUERY_HEADS * HEAD_WIDTH),
            key_total_sum.reshape(sequence_total, KEY_VALUE_HEADS * HEAD_WIDTH).astype(jnp.bfloat16),
            value_total_sum.reshape(sequence_total, KEY_VALUE_HEADS * HEAD_WIDTH).astype(jnp.bfloat16))


def reference(query_matrix, key_matrix, value_matrix, output_gradient, hidden_in, doc_lengths, querya, queryb, valuea, valueb):
    query_grad, key_grad, value_gradient = lax.map(sequence_grads, (query_matrix, key_matrix, value_matrix, output_gradient, doc_lengths))
    tokens_in = hidden_in.reshape(-1, D)
    flat_query = query_grad.reshape(-1, QUERY_HEADS * HEAD_WIDTH)
    flattened_value = value_gradient.reshape(-1, KEY_VALUE_HEADS * HEAD_WIDTH)
    query_proj = contract_last(tokens_in, querya).astype(jnp.bfloat16)
    value_proj = contract_last(tokens_in, valuea).astype(jnp.bfloat16)
    query_low = contract_last(flat_query, queryb).astype(jnp.bfloat16)
    value_low = contract_last(flattened_value, valueb).astype(jnp.bfloat16)
    querya_grad = ADAPTER_SCALE * contract_first(query_low, tokens_in)
    queryb_grad = ADAPTER_SCALE * contract_first(query_proj, flat_query)
    valuea_grad = ADAPTER_SCALE * contract_first(value_low, tokens_in)
    valueb_grad = ADAPTER_SCALE * contract_first(value_proj, flattened_value)
    return (query_grad, key_grad, value_gradient, querya_grad, queryb_grad, valuea_grad, valueb_grad)
```

```python
import math

import jax
import jax.numpy as jnp
from jax import lax
from jax.experimental import pallas as pl
from jax.experimental.pallas import tpu as pltpu
from jax.sharding import PartitionSpec as P

MESH = pl.DeviceIdType.MESH
HEAD = 128
GROUP = 4
TOK = 128
RING = 8
CHIP_ROWS = 256
HALF_SEQ = 2048
SEQ = 4096
KB = 256
NKB = SEQ // KB
RANK = 16
PACKED = 12288
CORE_COLS = PACKED // 2
Z_COLS = CORE_COLS // RING
DOCS = 16
NEG = -1e30
SCALE = HEAD ** (-0.5)
LOG2E = math.log2(math.e)
ANY = pl.BlockSpec(memory_space=pl.ANY)
VMEM = pl.BlockSpec(memory_space=pltpu.VMEM)
SMEM = pl.BlockSpec(memory_space=pltpu.SMEM)


def nn(left, right):
    return lax.dot_general(left, right, (((1,), (0,)), ((), ())), preferred_element_type=jnp.float32)


def nt(left, right):
    return lax.dot_general(left, right, (((1,), (1,)), ((), ())), preferred_element_type=jnp.float32)


def place():
    me = lax.axis_index("ctx")
    return me // 16, (me // 2) % RING, me % 2


def ctx_of(a, z, c):
    return a * 16 + z * 2 + c


def mult(value, of):
    return pl.multiple_of(value, of)


def group_peers(a, c):
    return ((a, 1 - c), (1 - a, c), (1 - a, 1 - c))


def enter(ids):
    barrier = pltpu.get_barrier_semaphore()
    for one in ids:
        pl.semaphore_signal(barrier, inc=1, device_id=one, device_id_type=MESH)
    pl.semaphore_wait(barrier, len(ids))


def remote(src, dst, ssem, rsem, to):
    return pltpu.make_async_remote_copy(
        src_ref=src, dst_ref=dst, send_sem=ssem, recv_sem=rsem, device_id=to, device_id_type=MESH
    )


def ring_and_group(a, z, c):
    ids = [{"ctx": ctx_of(pa, z, pc)} for pa, pc in group_peers(a, c)]
    ids.append({"ctx": ctx_of(a, (z + 1) % RING, c)})
    ids.append({"ctx": ctx_of(a, (z + RING - 1) % RING, c)})
    return ids


def gather_kernel(q_ref, do_ref, k_ref, v_ref, qg_ref, dog_ref, kg_ref, vg_ref,
                  kall, vall, qst, dost, gs, gr, xs, xr, rs, rr, ls):
    a, z, c = place()
    ids = ring_and_group(a, z, c)
    own = 2 * a + c
    row0 = mult(a * HALF_SEQ + z * CHIP_ROWS + c * TOK, TOK)
    local = []
    for i, (src, dst) in enumerate(((k_ref, kall), (v_ref, vall))):
        local.append(pltpu.make_async_copy(
            src.at[:, pl.ds(mult(own * HEAD, HEAD), HEAD)], dst.at[pl.ds(row0, TOK)], ls.at[i]))
    wide = []
    for i, (src, dst) in enumerate(((q_ref, qst), (do_ref, dost))):
        wide.append(pltpu.make_async_copy(
            src.at[:, pl.ds(mult(own * 512, 512), 512)], dst, ls.at[2 + i]))
    for one in local + wide:
        one.start()
    enter(ids)
    sent = []
    peers = group_peers(a, c)
    for p, (pa, pc) in enumerate(peers):
        for i, (src, dst) in enumerate(((k_ref, kall), (v_ref, vall))):
            head = 2 * pa + pc
            cp = remote(src.at[:, pl.ds(mult(head * HEAD, HEAD), HEAD)], dst.at[pl.ds(row0, TOK)],
                        gs.at[2 * p + i], gr.at[2 * p + i], ids[p])
            cp.start()
            sent.append(cp)
    for p, (pa, pc) in enumerate(peers):
        for i, (src, dst) in enumerate(((q_ref, qg_ref), (do_ref, dog_ref))):
            head = 2 * pa + pc
            cp = remote(src.at[:, pl.ds(mult(head * 512, 512), 512)],
                        dst.at[pl.ds(mult(own * TOK, TOK), TOK)],
                        xs.at[2 * p + i], xr.at[2 * p + i], ids[p])
            cp.start()
            sent.append(cp)

    def group_arrived(p):
        pa, pc = peers[p]
        rows = pl.ds(mult(pa * HALF_SEQ + z * CHIP_ROWS + pc * TOK, TOK), TOK)
        for i, dst in enumerate((kall, vall)):
            remote(dst.at[rows], dst.at[rows], gs.at[2 * p + i], gr.at[2 * p + i], ids[p]).wait_recv()

    chunks = ((kall, a), (vall, a), (kall, 1 - a), (vall, 1 - a))
    ways = (1, -1)

    def chunk(j, zz):
        ref, y = chunks[j]
        return ref.at[pl.ds(mult(y * HALF_SEQ + zz * CHIP_ROWS, CHIP_ROWS), CHIP_ROWS)]

    def at(w, s, j):
        return (w * 4 + s) * 4 + j

    def send_on(w, s, j):
        part = chunk(j, (z + 2 * RING - ways[w] * s) % RING)
        cp = remote(part, part, rs.at[at(w, s, j)], rr.at[at(w, s, j)], ids[3 + w])
        cp.start()
        sent.append(cp)

    def arrived(w, s, j):
        part = chunk(j, (z + 2 * RING - ways[w] * (s + 1)) % RING)
        remote(part, part, rs.at[at(w, s, j)], rr.at[at(w, s, j)], ids[3 + w]).wait_recv()

    def carries(w, s, j):
        return s < 3 or (j < 2) == (w == 0)

    for one in local:
        one.wait()
    group_arrived(0)
    for j in (0, 1):
        for w in (0, 1):
            send_on(w, 0, j)
    group_arrived(1)
    group_arrived(2)
    for j in (2, 3):
        for w in (0, 1):
            send_on(w, 0, j)
    for s in range(4):
        for j in range(4):
            for w in (0, 1):
                if carries(w, s, j):
                    arrived(w, s, j)
                    if s < 3 and carries(w, s + 1, j):
                        send_on(w, s + 1, j)
    out = []
    for i, (src, dst) in enumerate(((kall, kg_ref), (vall, vg_ref))):
        out.append(pltpu.make_async_copy(src, dst, ls.at[i]))
    for one in wide:
        one.wait()
    for i, (src, dst) in enumerate(((qst, qg_ref), (dost, dog_ref))):
        out.append(pltpu.make_async_copy(src, dst.at[pl.ds(mult(own * TOK, TOK), TOK)], ls.at[2 + i]))
    for one in out:
        one.start()
    for p, (pa, pc) in enumerate(peers):
        rows = pl.ds(mult((2 * pa + pc) * TOK, TOK), TOK)
        for i, dst in enumerate((qg_ref, dog_ref)):
            remote(dst.at[rows], dst.at[rows], xs.at[2 * p + i], xr.at[2 * p + i], ids[p]).wait_recv()
    for one in out:
        one.wait()
    for one in sent:
        one.wait_send()


def gather_call(q, do, k, v):
    bf = jnp.bfloat16
    dma = pltpu.SemaphoreType.DMA
    return pl.pallas_call(
        gather_kernel,
        out_shape=(
            jax.ShapeDtypeStruct((512, 512), bf), jax.ShapeDtypeStruct((512, 512), bf),
            jax.ShapeDtypeStruct((SEQ, HEAD), bf), jax.ShapeDtypeStruct((SEQ, HEAD), bf),
        ),
        in_specs=[ANY, ANY, VMEM, VMEM],
        out_specs=(ANY, ANY, ANY, ANY),
        scratch_shapes=[
            pltpu.VMEM((SEQ, HEAD), bf), pltpu.VMEM((SEQ, HEAD), bf),
            pltpu.VMEM((TOK, 512), bf), pltpu.VMEM((TOK, 512), bf),
            dma((6,)), dma((6,)), dma((6,)), dma((6,)), dma((32,)), dma((32,)), dma((4,)),
        ],
        compiler_params=pltpu.CompilerParams(collective_id=0, has_side_effects=True),
        name="gather",
    )(q, do, k, v)


def attend_kernel(len_ref, q_ref, do_ref, k_ref, v_ref, dq_ref, dk_ref, dv_ref,
                  s_ref, kt, vt, qs, dos, dot_ref, ot, dqt, dka, dva):
    _, z, _ = place()
    bf, f32 = jnp.bfloat16, jnp.float32
    fold = SCALE * LOG2E

    def prepare(b, carry):
        rows = pl.ds(mult(b * KB, KB), KB)
        kt[b] = k_ref[rows, :].T
        vt[b] = v_ref[rows, :].T
        dka[b] = jnp.zeros((KB, HEAD), f32)
        dva[b] = jnp.zeros((KB, HEAD), f32)
        return carry

    lax.fori_loop(0, NKB, prepare, 0)
    starts = [jnp.int32(0)]
    for d in range(DOCS - 1):
        starts.append(starts[-1] + len_ref[0, d])

    def tile(t, carry):
        first = (t // 2) * HALF_SEQ + z * CHIP_ROWS + (t % 2) * TOK
        rows = pl.ds(mult(t * TOK, TOK), TOK)
        for h in range(GROUP):
            part = slice(h * HEAD, (h + 1) * HEAD)
            qs[part, :] = q_ref[rows, part]
            grads = do_ref[rows, part]
            dos[part, :] = grads
            dot_ref[:, part] = grads.astype(f32).T
        query_pos = first + lax.broadcasted_iota(jnp.int32, (1, 512), 1) % TOK
        begin = jnp.zeros((1, 512), jnp.int32)
        low = jnp.int32(0)
        for at in starts:
            begin = jnp.where(at <= query_pos, jnp.maximum(begin, at), begin)
            low = jnp.where(at <= first, jnp.maximum(low, at), low)
        kb0 = low // KB
        kb1 = first // KB + 1

        def score(b, top):
            keys = k_ref[pl.ds(mult(b * KB, KB), KB), :]
            s = nt(keys, qs[...])
            key_pos = b * KB + lax.broadcasted_iota(jnp.int32, (KB, 512), 0)
            s = jnp.where((key_pos >= begin) & (key_pos <= query_pos), s, NEG)
            s_ref[b] = s
            return jnp.maximum(top, jnp.max(s, axis=0, keepdims=True))

        top = lax.fori_loop(kb0, kb1, score, jnp.full((1, 512), NEG, f32)) * fold
        ot[...] = jnp.zeros_like(ot)

        def weigh(b, total):
            e = jnp.exp2(s_ref[b] * fold - top)
            s_ref[b] = e
            ot[...] += nn(vt[b], e.astype(bf))
            return total + jnp.sum(e, axis=0, keepdims=True)

        total = lax.fori_loop(kb0, kb1, weigh, jnp.zeros((1, 512), f32))
        inverse = 1.0 / total
        delta = jnp.sum(dot_ref[...] * ot[...], axis=0, keepdims=True) * inverse
        dqt[...] = jnp.zeros_like(dqt)

        def back(b, carry):
            values = v_ref[pl.ds(mult(b * KB, KB), KB), :]
            p = s_ref[b] * inverse
            gp = nt(values, dos[...])
            ds = (p * (gp - delta)).astype(bf)
            dva[b] += nn(p.astype(bf), dos[...])
            dka[b] += nn(ds, qs[...])
            dqt[...] += nn(kt[b], ds)
            return carry

        lax.fori_loop(kb0, kb1, back, 0)
        for h in range(GROUP):
            part = slice(h * HEAD, (h + 1) * HEAD)
            dq_ref[rows, part] = (dqt[:, part] * SCALE).T.astype(bf)
        return carry

    lax.fori_loop(0, GROUP, tile, 0)

    def finish(b, carry):
        rows = pl.ds(mult(b * KB, KB), KB)
        dk_ref[rows, :] = (dka[b] * SCALE).astype(bf)
        dv_ref[rows, :] = dva[b].astype(bf)
        return carry

    lax.fori_loop(0, NKB, finish, 0)


def attend_call(lengths, q, do, k, v):
    bf, f32 = jnp.bfloat16, jnp.float32
    return pl.pallas_call(
        attend_kernel,
        out_shape=(
            jax.ShapeDtypeStruct((512, 512), bf),
            jax.ShapeDtypeStruct((SEQ, HEAD), bf), jax.ShapeDtypeStruct((SEQ, HEAD), bf),
        ),
        in_specs=[SMEM, VMEM, VMEM, VMEM, VMEM],
        out_specs=(VMEM, VMEM, VMEM),
        scratch_shapes=[
            pltpu.VMEM((NKB, KB, 512), f32),
            pltpu.VMEM((NKB, HEAD, KB), bf), pltpu.VMEM((NKB, HEAD, KB), bf),
            pltpu.VMEM((512, HEAD), bf), pltpu.VMEM((512, HEAD), bf),
            pltpu.VMEM((HEAD, 512), f32), pltpu.VMEM((HEAD, 512), f32), pltpu.VMEM((HEAD, 512), f32),
            pltpu.VMEM((NKB, KB, HEAD), f32), pltpu.VMEM((NKB, KB, HEAD), f32),
        ],
        compiler_params=pltpu.CompilerParams(vmem_limit_bytes=48 << 20),
        name="attend",
    )(lengths, q, do, k, v)


def reduce_kernel(dq_ref, dk_ref, dv_ref, hid_ref, qa_ref, qb_ref, va_ref, vb_ref,
                  dql_out, dkl_out, dvl_out, part_out,
                  rb, fin, dql, dkl, dvl, gs, gr, xs, xr, rs, rr, ls):
    bf, f32 = jnp.bfloat16, jnp.float32
    a, z, c = place()
    ids = ring_and_group(a, z, c)
    own = 2 * a + c
    peers = group_peers(a, c)
    ways = (1, -1)
    chunks = ((dk_ref, 1 - a), (dv_ref, 1 - a), (dk_ref, a), (dv_ref, a))
    head_cols = pl.ds(mult(own * HEAD, HEAD), HEAD)
    wide_cols = pl.ds(mult(own * 512, 512), 512)
    mine = pltpu.make_async_copy(
        dq_ref.at[pl.ds(mult(own * TOK, TOK), TOK)], dql.at[:, wide_cols], ls.at[0])
    mine.start()
    enter(ids)
    sent = []

    def rows_of(j, dist):
        y = chunks[j][1]
        return pl.ds(mult(y * HALF_SEQ + ((z + 2 * RING + dist) % RING) * CHIP_ROWS, CHIP_ROWS), CHIP_ROWS)

    def at(w, d, j):
        return (w * 4 + d - 1) * 4 + j

    def starts_far(w, j):
        return (j < 2) == (w == 0)

    def send_on(w, d, j, src):
        cp = remote(src, rb.at[at(w, d, j)], rs.at[at(w, d, j)], rr.at[at(w, d, j)], ids[3 + w])
        cp.start()
        sent.append(cp)

    def arrived(w, d, j):
        slot = rb.at[at(w, d, j)]
        remote(slot, slot, rs.at[at(w, d, j)], rr.at[at(w, d, j)], ids[3 + w]).wait_recv()

    for j in range(4):
        for w in (0, 1):
            if starts_far(w, j):
                send_on(w, 4, j, chunks[j][0].at[rows_of(j, 4)])
    for j in range(4):
        for w in (0, 1):
            if not starts_far(w, j):
                send_on(w, 3, j, chunks[j][0].at[rows_of(j, 3 * ways[w])])
    for p, (pa, pc) in enumerate(peers):
        cp = remote(dq_ref.at[pl.ds(mult((2 * pa + pc) * TOK, TOK), TOK)], dql.at[:, wide_cols],
                    xs.at[p], xr.at[p], ids[p])
        cp.start()
        sent.append(cp)
    hidden = hid_ref[...]
    query_proj = nt(qa_ref[...], hidden).astype(bf)
    value_proj = nt(va_ref[...], hidden).astype(bf)

    def forward(d):
        for j in range(4):
            for w in (0, 1):
                if d == 3 and not starts_far(w, j):
                    continue
                arrived(w, d + 1, j)
                slot = at(w, d + 1, j)
                own_part = chunks[j][0][rows_of(j, d * ways[w]), :].astype(f32)
                rb[slot] = (rb[slot].astype(f32) + own_part).astype(bf)
                send_on(w, d, j, rb.at[slot])

    forward(3)
    forward(2)
    mine.wait()
    for p, (pa, pc) in enumerate(peers):
        cols = pl.ds(mult((2 * pa + pc) * 512, 512), 512)
        remote(dql.at[:, cols], dql.at[:, cols], xs.at[p], xr.at[p], ids[p]).wait_recv()
    query = dql[...]
    dql_out[...] = query
    part_out[:, 4096:6144] = (2.0 * nn(query_proj, query)).astype(bf)
    query_low = nt(qb_ref[...], query).astype(bf)
    part_out[:, 0:4096] = (2.0 * nn(query_low, hidden)).astype(bf)
    forward(1)
    for j in range(4):
        for w in (0, 1):
            arrived(w, 1, j)
        both = rb[at(0, 1, j)].astype(f32) + rb[at(1, 1, j)].astype(f32)
        fin[j] = (both + chunks[j][0][rows_of(j, 0), :].astype(f32)).astype(bf)
        if j == 1:
            for i, dst in enumerate((dkl, dvl)):
                for p in (1, 2):
                    cp = remote(fin.at[i, pl.ds(mult(peers[p][1] * TOK, TOK), TOK)], dst.at[:, head_cols],
                                gs.at[2 * p + i], gr.at[2 * p + i], ids[p])
                    cp.start()
                    sent.append(cp)
    keep = []
    for i, dst in enumerate((dkl, dvl)):
        cp = remote(fin.at[2 + i, pl.ds(mult((1 - c) * TOK, TOK), TOK)], dst.at[:, head_cols],
                    gs.at[i], gr.at[i], ids[0])
        cp.start()
        sent.append(cp)
        one = pltpu.make_async_copy(
            fin.at[2 + i, pl.ds(mult(c * TOK, TOK), TOK)], dst.at[:, head_cols], ls.at[1 + i])
        one.start()
        keep.append(one)
    for one in keep:
        one.wait()
    for p, (pa, pc) in enumerate(peers):
        cols = pl.ds(mult((2 * pa + pc) * HEAD, HEAD), HEAD)
        for i, dst in enumerate((dkl, dvl)):
            remote(dst.at[:, cols], dst.at[:, cols], gs.at[2 * p + i], gr.at[2 * p + i], ids[p]).wait_recv()
    dkl_out[...] = dkl[...]
    value = dvl[...]
    dvl_out[...] = value
    part_out[:, 10240:10752] = (2.0 * nn(value_proj, value)).astype(bf)
    value_low = nt(vb_ref[...], value).astype(bf)
    part_out[:, 6144:10240] = (2.0 * nn(value_low, hidden)).astype(bf)
    part_out[:, 10752:PACKED] = jnp.zeros((RANK, PACKED - 10752), bf)
    for one in sent:
        one.wait_send()


def reduce_call(dq, dk, dv, hidden, qa, qb, va, vb):
    bf = jnp.bfloat16
    dma = pltpu.SemaphoreType.DMA
    return pl.pallas_call(
        reduce_kernel,
        out_shape=(
            jax.ShapeDtypeStruct((TOK, 2048), bf), jax.ShapeDtypeStruct((TOK, 512), bf),
            jax.ShapeDtypeStruct((TOK, 512), bf), jax.ShapeDtypeStruct((RANK, PACKED), bf),
        ),
        in_specs=[VMEM] * 8,
        out_specs=(VMEM,) * 4,
        scratch_shapes=[
            pltpu.VMEM((32, CHIP_ROWS, HEAD), bf), pltpu.VMEM((4, CHIP_ROWS, HEAD), bf),
            pltpu.VMEM((TOK, 2048), bf), pltpu.VMEM((TOK, 512), bf), pltpu.VMEM((TOK, 512), bf),
            dma((6,)), dma((6,)), dma((3,)), dma((3,)), dma((32,)), dma((32,)), dma((3,)),
        ],
        compiler_params=pltpu.CompilerParams(
            collective_id=1, has_side_effects=True, vmem_limit_bytes=40 << 20),
        name="reduce",
    )(dq, dk, dv, hidden, qa, qb, va, vb)


SPANS = ((0, 4096), (4096, 6144), (6144, 10240), (10240, 10752))


def total_kernel(part_ref, qa_out, qb_out, va_out, vb_out,
                 in1, h1, in2, h2, in3, full, s1, r1, s2, r2, s3, r3, s4, r4, s5, r5, ls):
    bf, f32 = jnp.bfloat16, jnp.float32
    a, z, c = place()
    seat = lax.axis_index("dp") * 2 + a
    sibling = {"ctx": ctx_of(a, z, 1 - c)}
    z_of = [(z + d) % RING for d in range(RING)]
    z_ids = [{"ctx": ctx_of(a, zz, c)} for zz in z_of]
    seats = [(seat + e) % 16 for e in range(16)]
    seat_ids = [{"dp": m // 2, "ctx": ctx_of(m % 2, z, c)} for m in seats]
    enter([sibling] + z_ids[1:] + seat_ids[1:])
    sent = []

    def half(which):
        return pl.ds(mult(which * CORE_COLS, CORE_COLS), CORE_COLS)

    one = remote(part_ref.at[:, half(1 - c)], in1, s1, r1, sibling)
    one.start()
    one.wait()
    h1[...] = (part_ref[:, half(c)].astype(f32) + in1[...].astype(f32)).astype(bf)

    def shard(zz):
        return pl.ds(mult(zz * Z_COLS, Z_COLS), Z_COLS)

    copies = []
    for d in range(1, RING):
        one = remote(h1.at[:, shard(z_of[d])], in2.at[d - 1], s2.at[d - 1], r2.at[d - 1], z_ids[d])
        one.start()
        copies.append(one)
    subtotal = h1[:, shard(z)].astype(f32)
    for d in range(1, RING):
        copies[d - 1].wait_recv()
        subtotal = subtotal + in2[d - 1].astype(f32)
    h2[...] = subtotal.astype(bf)
    sent += copies
    copies = []
    for e in range(1, 16):
        one = remote(h2, in3.at[seat], s3.at[e - 1], r3.at[e - 1], seat_ids[e])
        one.start()
        copies.append(one)
    in3[seat] = subtotal.astype(bf)
    for e in range(1, 16):
        slot = in3.at[(seat + 16 - e) % 16]
        remote(slot, slot, s3.at[e - 1], r3.at[e - 1], seat_ids[e]).wait_recv()
    subtotal = in3[0].astype(f32)
    for m in range(1, 16):
        subtotal = subtotal + in3[m].astype(f32)
    sent += copies
    full[c, z] = subtotal.astype(bf)
    copies = []
    for d in range(1, RING):
        one = remote(full.at[c, z], full.at[c, z], s4.at[d - 1], r4.at[d - 1], z_ids[d])
        one.start()
        copies.append(one)
    for d in range(1, RING):
        slot = full.at[c, (z + RING - d) % RING]
        remote(slot, slot, s4.at[d - 1], r4.at[d - 1], z_ids[d]).wait_recv()
    sent += copies
    one = remote(full.at[c], full.at[c], s5, r5, sibling)
    one.start()
    remote(full.at[1 - c], full.at[1 - c], s5, r5, sibling).wait_recv()
    sent.append(one)
    for out, (begin, end) in zip((qa_out, qb_out, va_out, vb_out), SPANS):
        for cc in range(2):
            for zz in range(RING):
                lo = cc * CORE_COLS + zz * Z_COLS
                x, y = max(lo, begin), min(lo + Z_COLS, end)
                if x < y:
                    out[:, x - begin:y - begin] = full[cc, zz, :, x - lo:y - lo].astype(f32)
    for one in sent:
        one.wait_send()


def total_call(part):
    bf, f32 = jnp.bfloat16, jnp.float32
    dma = pltpu.SemaphoreType.DMA
    return pl.pallas_call(
        total_kernel,
        out_shape=tuple(jax.ShapeDtypeStruct((RANK, e - b), f32) for b, e in SPANS),
        in_specs=[VMEM],
        out_specs=(VMEM,) * 4,
        scratch_shapes=[
            pltpu.VMEM((RANK, CORE_COLS), bf), pltpu.VMEM((RANK, CORE_COLS), bf),
            pltpu.VMEM((RING - 1, RANK, Z_COLS), bf), pltpu.VMEM((RANK, Z_COLS), bf),
            pltpu.VMEM((16, RANK, Z_COLS), bf), pltpu.VMEM((2, RING, RANK, Z_COLS), bf),
            dma, dma, dma((7,)), dma((7,)), dma((15,)), dma((15,)), dma((7,)), dma((7,)), dma, dma,
            dma,
        ],
        compiler_params=pltpu.CompilerParams(collective_id=2, has_side_effects=True),
        name="total",
    )(part)


def shards(q, k, v, do, hidden, lengths, qa, qb, va, vb):
    qg, dog, kg, vg = gather_call(q[0], do[0], k[0], v[0])
    dq, dk, dv = attend_call(lengths, qg, dog, kg, vg)
    dql, dkl, dvl, part = reduce_call(dq, dk, dv, hidden[0], qa, qb, va, vb)
    sums = total_call(part)
    return (dql[None], dkl[None], dvl[None]) + tuple(sums)


def solution(mesh):
    token = P("dp", "ctx", None)
    return jax.shard_map(
        shards,
        mesh=mesh,
        in_specs=(token, token, token, token, token, P("dp", None), P(), P(), P(), P()),
        out_specs=(token, token, token, P(), P(), P(), P()),
        check_vma=False,
    )
```

```python
import math

import jax
import jax.numpy as jnp
from jax import lax
from jax.experimental import pallas as pl
from jax.experimental.pallas import tpu as pltpu
from jax.sharding import PartitionSpec as P

MESH = pl.DeviceIdType.MESH
HEAD = 128
GROUP = 4
TOK = 128
RING = 8
CHIP_ROWS = 256
HALF_SEQ = 2048
SEQ = 4096
KB = 256
WIDE = GROUP * CHIP_ROWS
NKB = SEQ // KB
RANK = 16
PACKED = 6144
CORE_COLS = PACKED // 2
Z_COLS = CORE_COLS // RING
DOCS = 16
NEG = -1e30
SCALE = HEAD ** (-0.5)
LOG2E = math.log2(math.e)
ANY = pl.BlockSpec(memory_space=pl.ANY)
VMEM = pl.BlockSpec(memory_space=pltpu.VMEM)
SMEM = pl.BlockSpec(memory_space=pltpu.SMEM)


def nn(left, right):
    return lax.dot_general(left, right, (((1,), (0,)), ((), ())), preferred_element_type=jnp.float32)


def nt(left, right):
    return lax.dot_general(left, right, (((1,), (1,)), ((), ())), preferred_element_type=jnp.float32)


def place():
    me = lax.axis_index("ctx")
    return me // 16, (me // 2) % RING, me % 2


def ctx_of(a, z, c):
    return a * 16 + z * 2 + c


def mult(value, of):
    return pl.multiple_of(value, of)


def group_peers(a, c):
    return ((a, 1 - c), (1 - a, c), (1 - a, 1 - c))


def enter(ids):
    barrier = pltpu.get_barrier_semaphore()
    for one in ids:
        pl.semaphore_signal(barrier, inc=1, device_id=one, device_id_type=MESH)
    pl.semaphore_wait(barrier, len(ids))


def remote(src, dst, ssem, rsem, to):
    return pltpu.make_async_remote_copy(
        src_ref=src, dst_ref=dst, send_sem=ssem, recv_sem=rsem, device_id=to, device_id_type=MESH
    )


def ring_and_group(a, z, c):
    ids = [{"ctx": ctx_of(pa, z, pc)} for pa, pc in group_peers(a, c)]
    ids.append({"ctx": ctx_of(a, (z + 1) % RING, c)})
    ids.append({"ctx": ctx_of(a, (z + RING - 1) % RING, c)})
    return ids


def gather_kernel(q_ref, do_ref, k_ref, v_ref, qg_ref, dog_ref, kg_ref, vg_ref,
                  kall, vall, qall, doall, gs, gr, xs, xr, rs, rr, ls):
    a, z, c = place()
    ids = ring_and_group(a, z, c)
    own = 2 * a + c
    row0 = mult(a * HALF_SEQ + z * CHIP_ROWS + c * TOK, TOK)
    local = []
    for i, (src, dst) in enumerate(((k_ref, kall), (v_ref, vall))):
        local.append(pltpu.make_async_copy(
            src.at[:, pl.ds(mult(own * HEAD, HEAD), HEAD)], dst.at[pl.ds(row0, TOK)], ls.at[i]))
    wide = []
    for i, (src, dst) in enumerate(((q_ref, qall), (do_ref, doall))):
        wide.append(pltpu.make_async_copy(
            src.at[:, pl.ds(mult(own * 512, 512), 512)],
            dst.at[pl.ds(mult(own * TOK, TOK), TOK)], ls.at[2 + i]))
    for one in local + wide:
        one.start()
    enter(ids)
    sent = []
    peers = group_peers(a, c)
    for p, (pa, pc) in enumerate(peers):
        for i, (src, dst) in enumerate(((k_ref, kall), (v_ref, vall))):
            head = 2 * pa + pc
            cp = remote(src.at[:, pl.ds(mult(head * HEAD, HEAD), HEAD)], dst.at[pl.ds(row0, TOK)],
                        gs.at[2 * p + i], gr.at[2 * p + i], ids[p])
            cp.start()
            sent.append(cp)
    for p, (pa, pc) in enumerate(peers):
        for i, (src, dst) in enumerate(((q_ref, qall), (do_ref, doall))):
            head = 2 * pa + pc
            cp = remote(src.at[:, pl.ds(mult(head * 512, 512), 512)],
                        dst.at[pl.ds(mult(own * TOK, TOK), TOK)],
                        xs.at[2 * p + i], xr.at[2 * p + i], ids[p])
            cp.start()
            sent.append(cp)

    def group_arrived(p):
        pa, pc = peers[p]
        rows = pl.ds(mult(pa * HALF_SEQ + z * CHIP_ROWS + pc * TOK, TOK), TOK)
        for i, dst in enumerate((kall, vall)):
            remote(dst.at[rows], dst.at[rows], gs.at[2 * p + i], gr.at[2 * p + i], ids[p]).wait_recv()

    chunks = ((kall, a), (vall, a), (kall, 1 - a), (vall, 1 - a))
    ways = (1, -1)

    def chunk(j, zz):
        ref, y = chunks[j]
        return ref.at[pl.ds(mult(y * HALF_SEQ + zz * CHIP_ROWS, CHIP_ROWS), CHIP_ROWS)]

    def at(w, s, j):
        return (w * 4 + s) * 4 + j

    def send_on(w, s, j):
        part = chunk(j, (z + 2 * RING - ways[w] * s) % RING)
        cp = remote(part, part, rs.at[at(w, s, j)], rr.at[at(w, s, j)], ids[3 + w])
        cp.start()
        sent.append(cp)

    def arrived(w, s, j):
        part = chunk(j, (z + 2 * RING - ways[w] * (s + 1)) % RING)
        remote(part, part, rs.at[at(w, s, j)], rr.at[at(w, s, j)], ids[3 + w]).wait_recv()

    def carries(w, s, j):
        return s < 3 or (j < 2) == (w == 0)

    for one in local:
        one.wait()
    group_arrived(0)
    for j in (0, 1):
        for w in (0, 1):
            send_on(w, 0, j)
    group_arrived(1)
    group_arrived(2)
    for j in (2, 3):
        for w in (0, 1):
            send_on(w, 0, j)
    for s in range(4):
        for j in range(4):
            for w in (0, 1):
                if carries(w, s, j):
                    arrived(w, s, j)
                    if s < 3 and carries(w, s + 1, j):
                        send_on(w, s + 1, j)
    kg_ref[...] = kall[...]
    vg_ref[...] = vall[...]
    for one in wide:
        one.wait()
    for p, (pa, pc) in enumerate(peers):
        rows = pl.ds(mult((2 * pa + pc) * TOK, TOK), TOK)
        for i, dst in enumerate((qall, doall)):
            remote(dst.at[rows], dst.at[rows], xs.at[2 * p + i], xr.at[2 * p + i], ids[p]).wait_recv()
    qg_ref[...] = qall[...]
    dog_ref[...] = doall[...]
    for one in sent:
        one.wait_send()


def gather_call(q, do, k, v):
    bf = jnp.bfloat16
    dma = pltpu.SemaphoreType.DMA
    return pl.pallas_call(
        gather_kernel,
        out_shape=(
            jax.ShapeDtypeStruct((512, 512), bf), jax.ShapeDtypeStruct((512, 512), bf),
            jax.ShapeDtypeStruct((SEQ, HEAD), bf), jax.ShapeDtypeStruct((SEQ, HEAD), bf),
        ),
        in_specs=[ANY, ANY, VMEM, VMEM],
        out_specs=(VMEM,) * 4,
        scratch_shapes=[
            pltpu.VMEM((SEQ, HEAD), bf), pltpu.VMEM((SEQ, HEAD), bf),
            pltpu.VMEM((512, 512), bf), pltpu.VMEM((512, 512), bf),
            dma((6,)), dma((6,)), dma((6,)), dma((6,)), dma((32,)), dma((32,)), dma((4,)),
        ],
        compiler_params=pltpu.CompilerParams(
            collective_id=0, has_side_effects=True, vmem_limit_bytes=14 << 20),
        name="gather",
    )(q, do, k, v)


def attend_kernel(len_ref, q_ref, do_ref, k_ref, v_ref, dq_ref, dk_ref, dv_ref,
                  s_ref, kt, vt, qs, dos, dot_ref, ot, dqt, dka, dva):
    _, z, _ = place()
    bf, f32 = jnp.bfloat16, jnp.float32
    fold = SCALE * LOG2E

    def prepare(b, carry):
        rows = pl.ds(mult(b * KB, KB), KB)
        kt[b] = k_ref[rows, :].T
        vt[b] = v_ref[rows, :].T
        dka[b] = jnp.zeros((KB, HEAD), f32)
        dva[b] = jnp.zeros((KB, HEAD), f32)
        return carry

    lax.fori_loop(0, NKB, prepare, 0)
    starts = [jnp.int32(0)]
    for d in range(DOCS - 1):
        starts.append(starts[-1] + len_ref[0, d])

    def tile(t, carry):
        first = t * HALF_SEQ + z * CHIP_ROWS
        rows = pl.ds(mult(t * CHIP_ROWS, CHIP_ROWS), CHIP_ROWS)
        for h in range(GROUP):
            part = slice(h * HEAD, (h + 1) * HEAD)
            stack = slice(h * CHIP_ROWS, (h + 1) * CHIP_ROWS)
            qs[stack, :] = q_ref[rows, part]
            grads = do_ref[rows, part]
            dos[stack, :] = grads
            dot_ref[:, stack] = grads.astype(f32).T
        query_pos = first + lax.broadcasted_iota(jnp.int32, (1, WIDE), 1) % CHIP_ROWS
        begin = jnp.zeros((1, WIDE), jnp.int32)
        low, high = jnp.int32(0), jnp.int32(0)
        for at in starts:
            begin = jnp.where(at <= query_pos, jnp.maximum(begin, at), begin)
            low = jnp.where(at <= first, jnp.maximum(low, at), low)
            high = jnp.where(at < first + CHIP_ROWS, jnp.maximum(high, at), high)
        kb0 = low // KB
        kb1 = first // KB + 1
        kbm = jnp.minimum((high + KB - 1) // KB, kb1 - 1)

        def score(b, top):
            keys = k_ref[pl.ds(mult(b * KB, KB), KB), :]
            s = nt(keys, qs[...])
            s_ref[b] = s
            return jnp.maximum(top, jnp.max(s, axis=0, keepdims=True))

        def score_masked(b, top):
            keys = k_ref[pl.ds(mult(b * KB, KB), KB), :]
            s = nt(keys, qs[...])
            key_pos = b * KB + lax.broadcasted_iota(jnp.int32, (KB, WIDE), 0)
            s = jnp.where((key_pos >= begin) & (key_pos <= query_pos), s, NEG)
            s_ref[b] = s
            return jnp.maximum(top, jnp.max(s, axis=0, keepdims=True))

        top = score_masked(kb1 - 1, jnp.full((1, WIDE), NEG, f32))
        top = lax.fori_loop(kb0, kbm, score_masked, top)
        top = lax.fori_loop(kbm, kb1 - 1, score, top) * fold
        ot[...] = jnp.zeros_like(ot)

        def weigh(b, total):
            e = jnp.exp2(s_ref[b] * fold - top)
            s_ref[b] = e
            ot[...] += nn(vt[b], e.astype(bf))
            return total + jnp.sum(e, axis=0, keepdims=True)

        total = lax.fori_loop(kb0, kb1, weigh, jnp.zeros((1, WIDE), f32))
        inverse = 1.0 / total
        delta = jnp.sum(dot_ref[...] * ot[...], axis=0, keepdims=True) * inverse
        dqt[...] = jnp.zeros_like(dqt)

        def back(b, carry):
            values = v_ref[pl.ds(mult(b * KB, KB), KB), :]
            p = s_ref[b] * inverse
            gp = nt(values, dos[...])
            ds = (p * (gp - delta)).astype(bf)
            dva[b] += nn(p.astype(bf), dos[...])
            dka[b] += nn(ds, qs[...])
            dqt[...] += nn(kt[b], ds)
            return carry

        lax.fori_loop(kb0, kb1, back, 0)
        for h in range(GROUP):
            part = slice(h * HEAD, (h + 1) * HEAD)
            stack = slice(h * CHIP_ROWS, (h + 1) * CHIP_ROWS)
            dq_ref[rows, part] = (dqt[:, stack] * SCALE).T.astype(bf)
        return carry

    lax.fori_loop(0, 2, tile, 0)

    def finish(b, carry):
        rows = pl.ds(mult(b * KB, KB), KB)
        dk_ref[rows, :] = (dka[b] * SCALE).astype(bf)
        dv_ref[rows, :] = dva[b].astype(bf)
        return carry

    lax.fori_loop(0, NKB, finish, 0)


def attend_call(lengths, q, do, k, v):
    bf, f32 = jnp.bfloat16, jnp.float32
    return pl.pallas_call(
        attend_kernel,
        out_shape=(
            jax.ShapeDtypeStruct((512, 512), bf),
            jax.ShapeDtypeStruct((SEQ, HEAD), bf), jax.ShapeDtypeStruct((SEQ, HEAD), bf),
        ),
        in_specs=[SMEM, VMEM, VMEM, VMEM, VMEM],
        out_specs=(VMEM, VMEM, VMEM),
        scratch_shapes=[
            pltpu.VMEM((NKB, KB, WIDE), f32),
            pltpu.VMEM((NKB, HEAD, KB), bf), pltpu.VMEM((NKB, HEAD, KB), bf),
            pltpu.VMEM((WIDE, HEAD), bf), pltpu.VMEM((WIDE, HEAD), bf),
            pltpu.VMEM((HEAD, WIDE), f32), pltpu.VMEM((HEAD, WIDE), f32), pltpu.VMEM((HEAD, WIDE), f32),
            pltpu.VMEM((NKB, KB, HEAD), f32), pltpu.VMEM((NKB, KB, HEAD), f32),
        ],
        compiler_params=pltpu.CompilerParams(vmem_limit_bytes=46 << 20),
        name="attend",
    )(lengths, q, do, k, v)


def reduce_kernel(dq_ref, dk_ref, dv_ref, hid_ref, qa_ref, qb_ref, va_ref, vb_ref,
                  dql_out, dkl_out, dvl_out, full_out,
                  rb, fin, dql, dkl, dvl, part, in1, h1, in2, h2, in3, full,
                  gs, gr, xs, xr, rs, rr, ls,
                  s1, r1, s2, r2, s3, r3, s4, r4, s5, r5):
    bf, f32 = jnp.bfloat16, jnp.float32
    a, z, c = place()
    ids = ring_and_group(a, z, c)
    own = 2 * a + c
    peers = group_peers(a, c)
    ways = (1, -1)
    chunks = ((dk_ref, 1 - a), (dv_ref, 1 - a), (dk_ref, a), (dv_ref, a))
    head_cols = pl.ds(mult(own * HEAD, HEAD), HEAD)
    wide_cols = pl.ds(mult(own * 512, 512), 512)
    seat = lax.axis_index("dp") * 2 + a
    sibling = ids[0]
    z_of = [(z + d) % RING for d in range(RING)]
    z_ids = [{"ctx": ctx_of(a, zz, c)} for zz in z_of]
    seats = [(seat + e) % 16 for e in range(16)]
    seat_ids = [{"dp": m // 2, "ctx": ctx_of(m % 2, z, c)} for m in seats]
    mine = pltpu.make_async_copy(
        dq_ref.at[pl.ds(mult(own * TOK, TOK), TOK)], dql.at[:, wide_cols], ls.at[0])
    mine.start()
    enter([sibling, ids[2]] + z_ids[1:] + seat_ids[1:])
    sent = []

    def go(src, dst, ssem, rsem, to):
        cp = remote(src, dst, ssem, rsem, to)
        cp.start()
        sent.append(cp)

    def came(dst, ssem, rsem, to):
        remote(dst, dst, ssem, rsem, to).wait_recv()

    def rows_of(j, dist):
        y = chunks[j][1]
        return pl.ds(mult(y * HALF_SEQ + ((z + 2 * RING + dist) % RING) * CHIP_ROWS, CHIP_ROWS), CHIP_ROWS)

    def at(w, d, j):
        return (w * 4 + d - 1) * 4 + j

    def starts_far(w, j):
        return (j < 2) == (w == 0)

    def send_on(w, d, j, src):
        k = at(w, d, j)
        go(src, rb.at[k], rs.at[k], rr.at[k], ids[3 + w])

    def arrived(w, d, j):
        k = at(w, d, j)
        came(rb.at[k], rs.at[k], rr.at[k], ids[3 + w])

    def half(which):
        return pl.ds(mult(which * CORE_COLS, CORE_COLS), CORE_COLS)

    def shard(zz):
        return pl.ds(mult(zz * Z_COLS, Z_COLS), Z_COLS)

    def core_send(u):
        go(part.at[u, :, half(1 - c)], in1.at[u], s1.at[u], r1.at[u], sibling)

    def z_send(u):
        came(in1.at[u], s1.at[u], r1.at[u], sibling)
        h1[u] = (part[u, :, half(c)].astype(f32) + in1[u].astype(f32)).astype(bf)
        for d in range(1, RING):
            k = u * 7 + d - 1
            go(h1.at[u, :, shard(z_of[d])], in2.at[k], s2.at[k], r2.at[k], z_ids[d])

    def seat_send(u):
        subtotal = h1[u, :, shard(z)].astype(f32)
        for d in range(1, RING):
            k = u * 7 + d - 1
            came(in2.at[k], s2.at[k], r2.at[k], z_ids[d])
            subtotal = subtotal + in2[k].astype(f32)
        h2[u] = subtotal.astype(bf)
        for e in range(1, 16):
            k = u * 15 + e - 1
            go(h2.at[u], in3.at[u, seat], s3.at[k], r3.at[k], seat_ids[e])
        in3[u, seat] = subtotal.astype(bf)

    def z_spread(u):
        for e in range(1, 16):
            k = u * 15 + e - 1
            came(in3.at[u, (seat + 16 - e) % 16], s3.at[k], r3.at[k], seat_ids[e])
        subtotal = in3[u, 0].astype(f32)
        for m in range(1, 16):
            subtotal = subtotal + in3[u, m].astype(f32)
        full[u, c, z] = subtotal.astype(bf)
        for d in range(1, RING):
            k = u * 7 + d - 1
            go(full.at[u, c, z], full.at[u, c, z], s4.at[k], r4.at[k], z_ids[d])

    def core_spread(u):
        for d in range(1, RING):
            k = u * 7 + d - 1
            came(full.at[u, c, (z + RING - d) % RING], s4.at[k], r4.at[k], z_ids[d])
        go(full.at[u, c], full.at[u, c], s5.at[u], r5.at[u], sibling)

    def collect(u):
        came(full.at[u, 1 - c], s5.at[u], r5.at[u], sibling)
        full_out[u] = full[u]

    for j in range(4):
        for w in (0, 1):
            if starts_far(w, j):
                send_on(w, 4, j, chunks[j][0].at[rows_of(j, 4)])
    for j in range(4):
        for w in (0, 1):
            if not starts_far(w, j):
                send_on(w, 3, j, chunks[j][0].at[rows_of(j, 3 * ways[w])])
    for p, (pa, pc) in enumerate(peers):
        go(dq_ref.at[pl.ds(mult((2 * pa + pc) * TOK, TOK), TOK)], dql.at[:, wide_cols],
           xs.at[p], xr.at[p], ids[p])
    hidden = hid_ref[...]
    query_proj = nt(qa_ref[...], hidden).astype(bf)
    value_proj = nt(va_ref[...], hidden).astype(bf)
    part[1, :, 4608:PACKED] = jnp.zeros((RANK, PACKED - 4608), bf)

    def forward(d):
        for j in range(4):
            for w in (0, 1):
                if d == 3 and not starts_far(w, j):
                    continue
                arrived(w, d + 1, j)
                slot = at(w, d + 1, j)
                own_part = chunks[j][0][rows_of(j, d * ways[w]), :].astype(f32)
                rb[slot] = (rb[slot].astype(f32) + own_part).astype(bf)
                send_on(w, d, j, rb.at[slot])

    forward(3)
    mine.wait()
    for p, (pa, pc) in enumerate(peers):
        cols = pl.ds(mult((2 * pa + pc) * 512, 512), 512)
        came(dql.at[:, cols], xs.at[p], xr.at[p], ids[p])
    query = dql[...]
    dql_out[...] = query
    part[0, :, 4096:6144] = (2.0 * nn(query_proj, query)).astype(bf)
    query_low = nt(qb_ref[...], query).astype(bf)
    part[0, :, 0:4096] = (2.0 * nn(query_low, hidden)).astype(bf)
    core_send(0)
    forward(2)
    z_send(0)
    forward(1)
    seat_send(0)
    for j in range(4):
        for w in (0, 1):
            arrived(w, 1, j)
        both = rb[at(0, 1, j)].astype(f32) + rb[at(1, 1, j)].astype(f32)
        fin[j] = (both + chunks[j][0][rows_of(j, 0), :].astype(f32)).astype(bf)
        if j == 1:
            for i, dst in ((1, dvl), (0, dkl)):
                for p in (1, 2):
                    go(fin.at[i, pl.ds(mult(peers[p][1] * TOK, TOK), TOK)], dst.at[:, head_cols],
                       gs.at[2 * p + i], gr.at[2 * p + i], ids[p])
    keep = []
    for i, dst in ((1, dvl), (0, dkl)):
        go(fin.at[2 + i, pl.ds(mult((1 - c) * TOK, TOK), TOK)], dst.at[:, head_cols],
           gs.at[i], gr.at[i], ids[0])
        one = pltpu.make_async_copy(
            fin.at[2 + i, pl.ds(mult(c * TOK, TOK), TOK)], dst.at[:, head_cols], ls.at[1 + i])
        one.start()
        keep.append(one)
    for one in keep:
        one.wait()

    def returned(i, dst):
        for p, (pa, pc) in enumerate(peers):
            cols = pl.ds(mult((2 * pa + pc) * HEAD, HEAD), HEAD)
            came(dst.at[:, cols], gs.at[2 * p + i], gr.at[2 * p + i], ids[p])

    returned(1, dvl)
    value = dvl[...]
    part[1, :, 4096:4608] = (2.0 * nn(value_proj, value)).astype(bf)
    value_low = nt(vb_ref[...], value).astype(bf)
    part[1, :, 0:4096] = (2.0 * nn(value_low, hidden)).astype(bf)
    core_send(1)
    dvl_out[...] = value
    z_send(1)
    z_spread(0)
    seat_send(1)
    core_spread(0)
    returned(0, dkl)
    dkl_out[...] = dkl[...]
    z_spread(1)
    collect(0)
    core_spread(1)
    collect(1)
    for one in sent:
        one.wait_send()


def reduce_call(dq, dk, dv, hidden, qa, qb, va, vb):
    bf = jnp.bfloat16
    dma = pltpu.SemaphoreType.DMA
    return pl.pallas_call(
        reduce_kernel,
        out_shape=(
            jax.ShapeDtypeStruct((TOK, 2048), bf), jax.ShapeDtypeStruct((TOK, 512), bf),
            jax.ShapeDtypeStruct((TOK, 512), bf),
            jax.ShapeDtypeStruct((2, 2, RING, RANK, Z_COLS), bf),
        ),
        in_specs=[VMEM] * 8,
        out_specs=(VMEM,) * 4,
        scratch_shapes=[
            pltpu.VMEM((32, CHIP_ROWS, HEAD), bf), pltpu.VMEM((4, CHIP_ROWS, HEAD), bf),
            pltpu.VMEM((TOK, 2048), bf), pltpu.VMEM((TOK, 512), bf), pltpu.VMEM((TOK, 512), bf),
            pltpu.VMEM((2, RANK, PACKED), bf), pltpu.VMEM((2, RANK, CORE_COLS), bf),
            pltpu.VMEM((2, RANK, CORE_COLS), bf), pltpu.VMEM((14, RANK, Z_COLS), bf),
            pltpu.VMEM((2, RANK, Z_COLS), bf), pltpu.VMEM((2, 16, RANK, Z_COLS), bf),
            pltpu.VMEM((2, 2, RING, RANK, Z_COLS), bf),
            dma((6,)), dma((6,)), dma((3,)), dma((3,)), dma((32,)), dma((32,)), dma((3,)),
            dma((2,)), dma((2,)), dma((14,)), dma((14,)), dma((30,)), dma((30,)),
            dma((14,)), dma((14,)), dma((2,)), dma((2,)),
        ],
        compiler_params=pltpu.CompilerParams(
            collective_id=1, has_side_effects=True, vmem_limit_bytes=24 << 20),
        name="reduce",
    )(dq, dk, dv, hidden, qa, qb, va, vb)


SPANS = ((0, 0, 4096), (0, 4096, 6144), (1, 0, 4096), (1, 4096, 4608))


def finish_kernel(dql_ref, dkl_ref, dvl_ref, full_ref, dq_out, dk_out, dv_out,
                  qa_out, qb_out, va_out, vb_out, sem):
    copies = []
    for i, (src, dst) in enumerate(((dql_ref, dq_out), (dkl_ref, dk_out), (dvl_ref, dv_out))):
        copies.append(pltpu.make_async_copy(src, dst, sem.at[i]))
    for one in copies:
        one.start()
    for out, (u, begin, end) in zip((qa_out, qb_out, va_out, vb_out), SPANS):
        for cc in range(2):
            for zz in range(RING):
                lo = cc * CORE_COLS + zz * Z_COLS
                x, y = max(lo, begin), min(lo + Z_COLS, end)
                if x < y:
                    out[:, x - begin:y - begin] = full_ref[u, cc, zz, :, x - lo:y - lo].astype(jnp.float32)
    for one in copies:
        one.wait()


def finish_call(dql, dkl, dvl, full):
    bf = jnp.bfloat16
    return pl.pallas_call(
        finish_kernel,
        out_shape=(
            jax.ShapeDtypeStruct((TOK, 2048), bf), jax.ShapeDtypeStruct((TOK, 512), bf),
            jax.ShapeDtypeStruct((TOK, 512), bf),
        ) + tuple(jax.ShapeDtypeStruct((RANK, e - b), jnp.float32) for _, b, e in SPANS),
        in_specs=[VMEM] * 4,
        out_specs=(ANY,) * 3 + (VMEM,) * 4,
        scratch_shapes=[pltpu.SemaphoreType.DMA((3,))],
        compiler_params=pltpu.CompilerParams(vmem_limit_bytes=8 << 20),
        name="finish",
    )(dql, dkl, dvl, full)


def shards(q, k, v, do, hidden, lengths, qa, qb, va, vb):
    qg, dog, kg, vg = gather_call(q[0], do[0], k[0], v[0])
    dq, dk, dv = attend_call(lengths, qg, dog, kg, vg)
    landed = reduce_call(dq, dk, dv, hidden[0], qa, qb, va, vb)
    out = finish_call(*landed)
    return (out[0][None], out[1][None], out[2][None]) + tuple(out[3:])


def solution(mesh):
    token = P("dp", "ctx", None)
    return jax.shard_map(
        shards,
        mesh=mesh,
        in_specs=(token, token, token, token, token, P("dp", None), P(), P(), P(), P()),
        out_specs=(token, token, token, P(), P(), P(), P()),
        check_vma=False,
    )
```

```python
import math

import jax
import jax.numpy as jnp
from jax import lax
from jax.experimental import pallas as pl
from jax.experimental.pallas import tpu as pltpu
from jax.sharding import PartitionSpec as P

MESH = pl.DeviceIdType.MESH
HEAD = 128
GROUP = 4
TOK = 128
RING = 8
CHIP_ROWS = 256
HALF_SEQ = 2048
SEQ = 4096
KB = 256
WIDE = GROUP * CHIP_ROWS
NKB = SEQ // KB
RANK = 16
PACKED = 6144
CORE_COLS = PACKED // 2
Z_COLS = CORE_COLS // RING
DOCS = 16
NEG = -1e30
SCALE = HEAD ** (-0.5)
LOG2E = math.log2(math.e)
ANY = pl.BlockSpec(memory_space=pl.ANY)
VMEM = pl.BlockSpec(memory_space=pltpu.VMEM)
HBM = pl.BlockSpec(memory_space=pltpu.HBM)


def nn(left, right):
    return lax.dot_general(left, right, (((1,), (0,)), ((), ())), preferred_element_type=jnp.float32)


def nt(left, right):
    return lax.dot_general(left, right, (((1,), (1,)), ((), ())), preferred_element_type=jnp.float32)


def place():
    me = lax.axis_index("ctx")
    return me // 16, (me // 2) % RING, me % 2


def ctx_of(a, z, c):
    return a * 16 + z * 2 + c


def mult(value, of):
    return pl.multiple_of(value, of)


def group_peers(a, c):
    return ((a, 1 - c), (1 - a, c), (1 - a, 1 - c))


def enter(ids):
    barrier = pltpu.get_barrier_semaphore()
    for one in ids:
        pl.semaphore_signal(barrier, inc=1, device_id=one, device_id_type=MESH)
    pl.semaphore_wait(barrier, len(ids))


def remote(src, dst, ssem, rsem, to):
    return pltpu.make_async_remote_copy(
        src_ref=src, dst_ref=dst, send_sem=ssem, recv_sem=rsem, device_id=to, device_id_type=MESH
    )


def ring_and_group(a, z, c):
    ids = [{"ctx": ctx_of(pa, z, pc)} for pa, pc in group_peers(a, c)]
    ids.append({"ctx": ctx_of(a, (z + 1) % RING, c)})
    ids.append({"ctx": ctx_of(a, (z + RING - 1) % RING, c)})
    return ids


def gather_kernel(q_ref, do_ref, k_ref, v_ref, qg_ref, dog_ref, kg_ref, vg_ref,
                  kall, vall, qall, doall, gs, gr, xs, xr, rs, rr, ls):
    a, z, c = place()
    ids = ring_and_group(a, z, c)
    own = 2 * a + c
    row0 = mult(a * HALF_SEQ + z * CHIP_ROWS + c * TOK, TOK)
    local = []
    for i, (src, dst) in enumerate(((k_ref, kall), (v_ref, vall))):
        local.append(pltpu.make_async_copy(
            src.at[:, pl.ds(mult(own * HEAD, HEAD), HEAD)], dst.at[pl.ds(row0, TOK)], ls.at[i]))
    wide = []
    for i, (src, dst) in enumerate(((q_ref, qall), (do_ref, doall))):
        wide.append(pltpu.make_async_copy(
            src.at[:, pl.ds(mult(own * 512, 512), 512)],
            dst.at[pl.ds(mult(own * TOK, TOK), TOK)], ls.at[2 + i]))
    for one in local + wide:
        one.start()
    enter(ids)
    sent = []
    peers = group_peers(a, c)
    for p, (pa, pc) in enumerate(peers):
        for i, (src, dst) in enumerate(((k_ref, kall), (v_ref, vall))):
            head = 2 * pa + pc
            cp = remote(src.at[:, pl.ds(mult(head * HEAD, HEAD), HEAD)], dst.at[pl.ds(row0, TOK)],
                        gs.at[2 * p + i], gr.at[2 * p + i], ids[p])
            cp.start()
            sent.append(cp)
    for p, (pa, pc) in enumerate(peers):
        for i, (src, dst) in enumerate(((q_ref, qall), (do_ref, doall))):
            head = 2 * pa + pc
            cp = remote(src.at[:, pl.ds(mult(head * 512, 512), 512)],
                        dst.at[pl.ds(mult(own * TOK, TOK), TOK)],
                        xs.at[2 * p + i], xr.at[2 * p + i], ids[p])
            cp.start()
            sent.append(cp)

    def group_arrived(p):
        pa, pc = peers[p]
        rows = pl.ds(mult(pa * HALF_SEQ + z * CHIP_ROWS + pc * TOK, TOK), TOK)
        for i, dst in enumerate((kall, vall)):
            remote(dst.at[rows], dst.at[rows], gs.at[2 * p + i], gr.at[2 * p + i], ids[p]).wait_recv()

    chunks = ((kall, a), (vall, a), (kall, 1 - a), (vall, 1 - a))
    ways = (1, -1)

    def chunk(j, zz):
        ref, y = chunks[j]
        return ref.at[pl.ds(mult(y * HALF_SEQ + zz * CHIP_ROWS, CHIP_ROWS), CHIP_ROWS)]

    def at(w, s, j):
        return (w * 4 + s) * 4 + j

    def send_on(w, s, j):
        part = chunk(j, (z + 2 * RING - ways[w] * s) % RING)
        cp = remote(part, part, rs.at[at(w, s, j)], rr.at[at(w, s, j)], ids[3 + w])
        cp.start()
        sent.append(cp)

    def arrived(w, s, j):
        part = chunk(j, (z + 2 * RING - ways[w] * (s + 1)) % RING)
        remote(part, part, rs.at[at(w, s, j)], rr.at[at(w, s, j)], ids[3 + w]).wait_recv()

    def carries(w, s, j):
        return s < 3 or (j < 2) == (w == 0)

    for one in local:
        one.wait()
    group_arrived(0)
    for j in (0, 1):
        for w in (0, 1):
            send_on(w, 0, j)
    group_arrived(1)
    group_arrived(2)
    for j in (2, 3):
        for w in (0, 1):
            send_on(w, 0, j)
    for s in range(4):
        for j in range(4):
            for w in (0, 1):
                if carries(w, s, j):
                    arrived(w, s, j)
                    if s < 3 and carries(w, s + 1, j):
                        send_on(w, s + 1, j)
    kg_ref[...] = kall[...]
    vg_ref[...] = vall[...]
    for one in wide:
        one.wait()
    for p, (pa, pc) in enumerate(peers):
        rows = pl.ds(mult((2 * pa + pc) * TOK, TOK), TOK)
        for i, dst in enumerate((qall, doall)):
            remote(dst.at[rows], dst.at[rows], xs.at[2 * p + i], xr.at[2 * p + i], ids[p]).wait_recv()
    qg_ref[...] = qall[...]
    dog_ref[...] = doall[...]
    for one in sent:
        one.wait_send()


def gather_call(q, do, k, v):
    bf = jnp.bfloat16
    dma = pltpu.SemaphoreType.DMA
    return pl.pallas_call(
        gather_kernel,
        out_shape=(
            jax.ShapeDtypeStruct((512, 512), bf), jax.ShapeDtypeStruct((512, 512), bf),
            jax.ShapeDtypeStruct((SEQ, HEAD), bf), jax.ShapeDtypeStruct((SEQ, HEAD), bf),
        ),
        in_specs=[HBM] * 4,
        out_specs=(VMEM,) * 4,
        scratch_shapes=[
            pltpu.VMEM((SEQ, HEAD), bf), pltpu.VMEM((SEQ, HEAD), bf),
            pltpu.VMEM((512, 512), bf), pltpu.VMEM((512, 512), bf),
            dma((6,)), dma((6,)), dma((6,)), dma((6,)), dma((32,)), dma((32,)), dma((4,)),
        ],
        compiler_params=pltpu.CompilerParams(
            collective_id=0, has_side_effects=True, vmem_limit_bytes=14 << 20),
        name="gather",
    )(q, do, k, v)


def attend_kernel(len_hbm, q_ref, do_ref, k_ref, v_ref, dq_ref, dk_ref, dv_ref,
                  s_ref, kt, vt, qs, dos, dot_ref, ot, dqt, dka, dva, len_ref, sem):
    lengths = pltpu.make_async_copy(len_hbm, len_ref, sem)
    lengths.start()
    _, z, _ = place()
    bf, f32 = jnp.bfloat16, jnp.float32
    fold = SCALE * LOG2E

    def prepare(b, carry):
        rows = pl.ds(mult(b * KB, KB), KB)
        kt[b] = k_ref[rows, :].T
        vt[b] = v_ref[rows, :].T
        dka[b] = jnp.zeros((KB, HEAD), f32)
        dva[b] = jnp.zeros((KB, HEAD), f32)
        return carry

    lax.fori_loop(0, NKB, prepare, 0)
    lengths.wait()
    starts = [jnp.int32(0)]
    for d in range(DOCS - 1):
        starts.append(starts[-1] + len_ref[0, d])

    def tile(t, carry):
        first = t * HALF_SEQ + z * CHIP_ROWS
        rows = pl.ds(mult(t * CHIP_ROWS, CHIP_ROWS), CHIP_ROWS)
        for h in range(GROUP):
            part = slice(h * HEAD, (h + 1) * HEAD)
            stack = slice(h * CHIP_ROWS, (h + 1) * CHIP_ROWS)
            qs[stack, :] = q_ref[rows, part]
            grads = do_ref[rows, part]
            dos[stack, :] = grads
            dot_ref[:, stack] = grads.astype(f32).T
        query_pos = first + lax.broadcasted_iota(jnp.int32, (1, WIDE), 1) % CHIP_ROWS
        begin = jnp.zeros((1, WIDE), jnp.int32)
        low, high = jnp.int32(0), jnp.int32(0)
        for at in starts:
            begin = jnp.where(at <= query_pos, jnp.maximum(begin, at), begin)
            low = jnp.where(at <= first, jnp.maximum(low, at), low)
            high = jnp.where(at < first + CHIP_ROWS, jnp.maximum(high, at), high)
        kb0 = low // KB
        kb1 = first // KB + 1
        kbm = jnp.minimum((high + KB - 1) // KB, kb1 - 1)

        def score(b, top):
            keys = k_ref[pl.ds(mult(b * KB, KB), KB), :]
            s = nt(keys, qs[...])
            s_ref[b] = s
            return jnp.maximum(top, jnp.max(s, axis=0, keepdims=True))

        def score_masked(b, top):
            keys = k_ref[pl.ds(mult(b * KB, KB), KB), :]
            s = nt(keys, qs[...])
            key_pos = b * KB + lax.broadcasted_iota(jnp.int32, (KB, WIDE), 0)
            s = jnp.where((key_pos >= begin) & (key_pos <= query_pos), s, NEG)
            s_ref[b] = s
            return jnp.maximum(top, jnp.max(s, axis=0, keepdims=True))

        top = score_masked(kb1 - 1, jnp.full((1, WIDE), NEG, f32))
        top = lax.fori_loop(kb0, kbm, score_masked, top)
        top = lax.fori_loop(kbm, kb1 - 1, score, top) * fold
        ot[...] = jnp.zeros_like(ot)

        def weigh(b, total):
            e = jnp.exp2(s_ref[b] * fold - top)
            s_ref[b] = e
            ot[...] += nn(vt[b], e.astype(bf))
            return total + jnp.sum(e, axis=0, keepdims=True)

        total = lax.fori_loop(kb0, kb1, weigh, jnp.zeros((1, WIDE), f32))
        inverse = 1.0 / total
        delta = jnp.sum(dot_ref[...] * ot[...], axis=0, keepdims=True) * inverse
        dqt[...] = jnp.zeros_like(dqt)

        def back(b, carry):
            values = v_ref[pl.ds(mult(b * KB, KB), KB), :]
            p = s_ref[b] * inverse
            gp = nt(values, dos[...])
            ds = (p * (gp - delta)).astype(bf)
            dva[b] += nn(p.astype(bf), dos[...])
            dka[b] += nn(ds, qs[...])
            dqt[...] += nn(kt[b], ds)
            return carry

        lax.fori_loop(kb0, kb1, back, 0)
        for h in range(GROUP):
            part = slice(h * HEAD, (h + 1) * HEAD)
            stack = slice(h * CHIP_ROWS, (h + 1) * CHIP_ROWS)
            dq_ref[rows, part] = (dqt[:, stack] * SCALE).T.astype(bf)
        return carry

    lax.fori_loop(0, 2, tile, 0)

    def finish(b, carry):
        rows = pl.ds(mult(b * KB, KB), KB)
        dk_ref[rows, :] = (dka[b] * SCALE).astype(bf)
        dv_ref[rows, :] = dva[b].astype(bf)
        return carry

    lax.fori_loop(0, NKB, finish, 0)


def attend_call(lengths, q, do, k, v):
    bf, f32 = jnp.bfloat16, jnp.float32
    return pl.pallas_call(
        attend_kernel,
        out_shape=(
            jax.ShapeDtypeStruct((512, 512), bf),
            jax.ShapeDtypeStruct((SEQ, HEAD), bf), jax.ShapeDtypeStruct((SEQ, HEAD), bf),
        ),
        in_specs=[HBM, VMEM, VMEM, VMEM, VMEM],
        out_specs=(VMEM, VMEM, VMEM),
        scratch_shapes=[
            pltpu.VMEM((NKB, KB, WIDE), f32),
            pltpu.VMEM((NKB, HEAD, KB), bf), pltpu.VMEM((NKB, HEAD, KB), bf),
            pltpu.VMEM((WIDE, HEAD), bf), pltpu.VMEM((WIDE, HEAD), bf),
            pltpu.VMEM((HEAD, WIDE), f32), pltpu.VMEM((HEAD, WIDE), f32), pltpu.VMEM((HEAD, WIDE), f32),
            pltpu.VMEM((NKB, KB, HEAD), f32), pltpu.VMEM((NKB, KB, HEAD), f32),
            pltpu.SMEM((1, DOCS), jnp.int32), pltpu.SemaphoreType.DMA,
        ],
        compiler_params=pltpu.CompilerParams(vmem_limit_bytes=46 << 20),
        name="attend",
    )(lengths, q, do, k, v)


def reduce_kernel(dq_ref, dk_ref, dv_ref, hid_ref, qa_ref, qb_ref, va_ref, vb_ref,
                  dql_out, dkl_out, dvl_out, full_out,
                  rb, fin, dql, dkl, dvl, part, in1, h1, in2, h2, in3, full,
                  gs, gr, xs, xr, rs, rr, ls,
                  s1, r1, s2, r2, s3, r3, s4, r4, s5, r5):
    bf, f32 = jnp.bfloat16, jnp.float32
    a, z, c = place()
    ids = ring_and_group(a, z, c)
    own = 2 * a + c
    peers = group_peers(a, c)
    ways = (1, -1)
    chunks = ((dv_ref, 1 - a), (dv_ref, a), (dk_ref, 1 - a), (dk_ref, a))
    head_cols = pl.ds(mult(own * HEAD, HEAD), HEAD)
    wide_cols = pl.ds(mult(own * 512, 512), 512)
    seat = lax.axis_index("dp") * 2 + a
    sibling = ids[0]
    z_of = [(z + d) % RING for d in range(RING)]
    z_ids = [{"ctx": ctx_of(a, zz, c)} for zz in z_of]
    seats = [(seat + e) % 16 for e in range(16)]
    seat_ids = [{"dp": m // 2, "ctx": ctx_of(m % 2, z, c)} for m in seats]
    mine = pltpu.make_async_copy(
        dq_ref.at[pl.ds(mult(own * TOK, TOK), TOK)], dql.at[:, wide_cols], ls.at[0])
    mine.start()
    enter([sibling, ids[2]] + z_ids[1:] + seat_ids[1:])
    sent = []

    def go(src, dst, ssem, rsem, to):
        cp = remote(src, dst, ssem, rsem, to)
        cp.start()
        sent.append(cp)

    def came(dst, ssem, rsem, to):
        remote(dst, dst, ssem, rsem, to).wait_recv()

    def rows_of(j, dist):
        y = chunks[j][1]
        return pl.ds(mult(y * HALF_SEQ + ((z + 2 * RING + dist) % RING) * CHIP_ROWS, CHIP_ROWS), CHIP_ROWS)

    def at(w, d, j):
        return (w * 4 + d - 1) * 4 + j

    def starts_far(w, j):
        return (j % 2 == 0) == (w == 0)

    def send_on(w, d, j, src):
        k = at(w, d, j)
        go(src, rb.at[k], rs.at[k], rr.at[k], ids[3 + w])

    def arrived(w, d, j):
        k = at(w, d, j)
        came(rb.at[k], rs.at[k], rr.at[k], ids[3 + w])

    def half(which):
        return pl.ds(mult(which * CORE_COLS, CORE_COLS), CORE_COLS)

    def shard(zz):
        return pl.ds(mult(zz * Z_COLS, Z_COLS), Z_COLS)

    def core_send(u):
        go(part.at[u, :, half(1 - c)], in1.at[u], s1.at[u], r1.at[u], sibling)

    def z_send(u):
        came(in1.at[u], s1.at[u], r1.at[u], sibling)
        h1[u] = (part[u, :, half(c)].astype(f32) + in1[u].astype(f32)).astype(bf)
        for d in range(1, RING):
            k = u * 7 + d - 1
            go(h1.at[u, :, shard(z_of[d])], in2.at[k], s2.at[k], r2.at[k], z_ids[d])

    def seat_send(u):
        subtotal = h1[u, :, shard(z)].astype(f32)
        for d in range(1, RING):
            k = u * 7 + d - 1
            came(in2.at[k], s2.at[k], r2.at[k], z_ids[d])
            subtotal = subtotal + in2[k].astype(f32)
        h2[u] = subtotal.astype(bf)
        for e in range(1, 16):
            k = u * 15 + e - 1
            go(h2.at[u], in3.at[u, seat], s3.at[k], r3.at[k], seat_ids[e])
        in3[u, seat] = subtotal.astype(bf)

    def z_spread(u):
        for e in range(1, 16):
            k = u * 15 + e - 1
            came(in3.at[u, (seat + 16 - e) % 16], s3.at[k], r3.at[k], seat_ids[e])
        subtotal = in3[u, 0].astype(f32)
        for m in range(1, 16):
            subtotal = subtotal + in3[u, m].astype(f32)
        full[u, c, z] = subtotal.astype(bf)
        for d in range(1, RING):
            k = u * 7 + d - 1
            go(full.at[u, c, z], full.at[u, c, z], s4.at[k], r4.at[k], z_ids[d])

    def core_spread(u):
        for d in range(1, RING):
            k = u * 7 + d - 1
            came(full.at[u, c, (z + RING - d) % RING], s4.at[k], r4.at[k], z_ids[d])
        go(full.at[u, c], full.at[u, c], s5.at[u], r5.at[u], sibling)

    def collect(u):
        came(full.at[u, 1 - c], s5.at[u], r5.at[u], sibling)
        full_out[u] = full[u]

    def first_sends(js):
        for d, far in ((4, True), (3, False)):
            for j in js:
                for w in (0, 1):
                    if starts_far(w, j) == far:
                        send_on(w, d, j, chunks[j][0].at[rows_of(j, d * ways[w])])

    def forward(d, js):
        for j in js:
            for w in (0, 1):
                if d == 3 and not starts_far(w, j):
                    continue
                arrived(w, d + 1, j)
                slot = at(w, d + 1, j)
                own_part = chunks[j][0][rows_of(j, d * ways[w]), :].astype(f32)
                rb[slot] = (rb[slot].astype(f32) + own_part).astype(bf)
                send_on(w, d, j, rb.at[slot])

    def last(i, dst):
        for j in (2 * i, 2 * i + 1):
            for w in (0, 1):
                arrived(w, 1, j)
            both = rb[at(0, 1, j)].astype(f32) + rb[at(1, 1, j)].astype(f32)
            fin[j] = (both + chunks[j][0][rows_of(j, 0), :].astype(f32)).astype(bf)
            for p in ((1, 2) if j % 2 == 0 else (0,)):
                go(fin.at[j, pl.ds(mult(peers[p][1] * TOK, TOK), TOK)], dst.at[:, head_cols],
                   gs.at[2 * p + i], gr.at[2 * p + i], ids[p])
        one = pltpu.make_async_copy(
            fin.at[2 * i + 1, pl.ds(mult(c * TOK, TOK), TOK)], dst.at[:, head_cols], ls.at[1 + i])
        one.start()
        return one

    def returned(i, dst, own_copy):
        own_copy.wait()
        for p, (pa, pc) in enumerate(peers):
            cols = pl.ds(mult((2 * pa + pc) * HEAD, HEAD), HEAD)
            came(dst.at[:, cols], gs.at[2 * p + i], gr.at[2 * p + i], ids[p])

    values, keys = (0, 1), (2, 3)
    first_sends(values)
    for p, (pa, pc) in enumerate(peers):
        go(dq_ref.at[pl.ds(mult((2 * pa + pc) * TOK, TOK), TOK)], dql.at[:, wide_cols],
           xs.at[p], xr.at[p], ids[p])
    hidden = hid_ref[...]
    query_proj = nt(qa_ref[...], hidden).astype(bf)
    value_proj = nt(va_ref[...], hidden).astype(bf)
    part[1, :, 4608:PACKED] = jnp.zeros((RANK, PACKED - 4608), bf)
    forward(3, values)
    forward(2, values)
    forward(1, values)
    first_sends(keys)
    own_values = last(0, dvl)
    mine.wait()
    for p, (pa, pc) in enumerate(peers):
        cols = pl.ds(mult((2 * pa + pc) * 512, 512), 512)
        came(dql.at[:, cols], xs.at[p], xr.at[p], ids[p])
    query = dql[...]
    part[0, :, 4096:6144] = (2.0 * nn(query_proj, query)).astype(bf)
    query_low = nt(qb_ref[...], query).astype(bf)
    part[0, :, 0:4096] = (2.0 * nn(query_low, hidden)).astype(bf)
    core_send(0)
    forward(3, keys)
    returned(0, dvl, own_values)
    value = dvl[...]
    part[1, :, 4096:4608] = (2.0 * nn(value_proj, value)).astype(bf)
    value_low = nt(vb_ref[...], value).astype(bf)
    part[1, :, 0:4096] = (2.0 * nn(value_low, hidden)).astype(bf)
    core_send(1)
    z_send(0)
    z_send(1)
    forward(2, keys)
    seat_send(0)
    seat_send(1)
    forward(1, keys)
    dql_out[...] = query
    dvl_out[...] = value
    z_spread(0)
    own_keys = last(1, dkl)
    z_spread(1)
    core_spread(0)
    returned(1, dkl, own_keys)
    dkl_out[...] = dkl[...]
    core_spread(1)
    collect(0)
    collect(1)
    for one in sent:
        one.wait_send()


def reduce_call(dq, dk, dv, hidden, qa, qb, va, vb):
    bf = jnp.bfloat16
    dma = pltpu.SemaphoreType.DMA
    return pl.pallas_call(
        reduce_kernel,
        out_shape=(
            jax.ShapeDtypeStruct((TOK, 2048), bf), jax.ShapeDtypeStruct((TOK, 512), bf),
            jax.ShapeDtypeStruct((TOK, 512), bf),
            jax.ShapeDtypeStruct((2, 2, RING, RANK, Z_COLS), bf),
        ),
        in_specs=[VMEM] * 8,
        out_specs=(VMEM,) * 4,
        scratch_shapes=[
            pltpu.VMEM((32, CHIP_ROWS, HEAD), bf), pltpu.VMEM((4, CHIP_ROWS, HEAD), bf),
            pltpu.VMEM((TOK, 2048), bf), pltpu.VMEM((TOK, 512), bf), pltpu.VMEM((TOK, 512), bf),
            pltpu.VMEM((2, RANK, PACKED), bf), pltpu.VMEM((2, RANK, CORE_COLS), bf),
            pltpu.VMEM((2, RANK, CORE_COLS), bf), pltpu.VMEM((14, RANK, Z_COLS), bf),
            pltpu.VMEM((2, RANK, Z_COLS), bf), pltpu.VMEM((2, 16, RANK, Z_COLS), bf),
            pltpu.VMEM((2, 2, RING, RANK, Z_COLS), bf),
            dma((6,)), dma((6,)), dma((3,)), dma((3,)), dma((32,)), dma((32,)), dma((3,)),
            dma((2,)), dma((2,)), dma((14,)), dma((14,)), dma((30,)), dma((30,)),
            dma((14,)), dma((14,)), dma((2,)), dma((2,)),
        ],
        compiler_params=pltpu.CompilerParams(
            collective_id=1, has_side_effects=True, vmem_limit_bytes=24 << 20),
        name="reduce",
    )(dq, dk, dv, hidden, qa, qb, va, vb)


SPANS = ((0, 0, 4096), (0, 4096, 6144), (1, 0, 4096), (1, 4096, 4608))


def finish_kernel(dql_ref, dkl_ref, dvl_ref, full_ref, dq_out, dk_out, dv_out,
                  qa_out, qb_out, va_out, vb_out, sem):
    copies = []
    for i, (src, dst) in enumerate(((dql_ref, dq_out), (dkl_ref, dk_out), (dvl_ref, dv_out))):
        copies.append(pltpu.make_async_copy(src, dst, sem.at[i]))
    for one in copies:
        one.start()
    for out, (u, begin, end) in zip((qa_out, qb_out, va_out, vb_out), SPANS):
        for cc in range(2):
            for zz in range(RING):
                lo = cc * CORE_COLS + zz * Z_COLS
                x, y = max(lo, begin), min(lo + Z_COLS, end)
                if x < y:
                    out[:, x - begin:y - begin] = full_ref[u, cc, zz, :, x - lo:y - lo].astype(jnp.float32)
    for one in copies:
        one.wait()


def finish_call(dql, dkl, dvl, full):
    bf = jnp.bfloat16
    return pl.pallas_call(
        finish_kernel,
        out_shape=(
            jax.ShapeDtypeStruct((TOK, 2048), bf), jax.ShapeDtypeStruct((TOK, 512), bf),
            jax.ShapeDtypeStruct((TOK, 512), bf),
        ) + tuple(jax.ShapeDtypeStruct((RANK, e - b), jnp.float32) for _, b, e in SPANS),
        in_specs=[VMEM] * 4,
        out_specs=(ANY,) * 3 + (VMEM,) * 4,
        scratch_shapes=[pltpu.SemaphoreType.DMA((3,))],
        compiler_params=pltpu.CompilerParams(vmem_limit_bytes=8 << 20),
        name="finish",
    )(dql, dkl, dvl, full)


def shards(q, k, v, do, hidden, lengths, qa, qb, va, vb):
    qg, dog, kg, vg = gather_call(q[0], do[0], k[0], v[0])
    dq, dk, dv = attend_call(lengths, qg, dog, kg, vg)
    landed = reduce_call(dq, dk, dv, hidden[0], qa, qb, va, vb)
    out = finish_call(*landed)
    return (out[0][None], out[1][None], out[2][None]) + tuple(out[3:])


def solution(mesh):
    token = P("dp", "ctx", None)
    return jax.shard_map(
        shards,
        mesh=mesh,
        in_specs=(token, token, token, token, token, P("dp", None), P(), P(), P(), P()),
        out_specs=(token, token, token, P(), P(), P(), P()),
        check_vma=False,
    )
```

```python
import math

import jax
import jax.numpy as jnp
from jax import lax
from jax.experimental import pallas as pl
from jax.experimental.pallas import tpu as pltpu
from jax.sharding import PartitionSpec as P

MESH = pl.DeviceIdType.MESH
HEAD = 128
GROUP = 4
TOK = 128
RING = 8
CHIP_ROWS = 256
HALF_SEQ = 2048
SEQ = 4096
KB = 256
WIDE = GROUP * CHIP_ROWS
PAIRS = SEQ // KB + HALF_SEQ // KB
FOLD = HEAD ** (-0.5) * math.log2(math.e)
NKB = SEQ // KB
RANK = 16
PACKED = 6144
CORE_COLS = PACKED // 2
Z_COLS = CORE_COLS // RING
DOCS = 16
NEG = -1e30
SCALE = HEAD ** (-0.5)
ANY = pl.BlockSpec(memory_space=pl.ANY)
VMEM = pl.BlockSpec(memory_space=pltpu.VMEM)
SMEM = pl.BlockSpec(memory_space=pltpu.SMEM)
HBM = pl.BlockSpec(memory_space=pltpu.HBM)


def nn(left, right):
    return lax.dot_general(left, right, (((1,), (0,)), ((), ())), preferred_element_type=jnp.float32)


def nt(left, right):
    return lax.dot_general(left, right, (((1,), (1,)), ((), ())), preferred_element_type=jnp.float32)


def place():
    me = lax.axis_index("ctx")
    return me // 16, (me // 2) % RING, me % 2


def ctx_of(a, z, c):
    return a * 16 + z * 2 + c


def mult(value, of):
    return pl.multiple_of(value, of)


def group_peers(a, c):
    return ((a, 1 - c), (1 - a, c), (1 - a, 1 - c))


def enter(ids):
    barrier = pltpu.get_barrier_semaphore()
    for one in ids:
        pl.semaphore_signal(barrier, inc=1, device_id=one, device_id_type=MESH)
    pl.semaphore_wait(barrier, len(ids))


def remote(src, dst, ssem, rsem, to):
    return pltpu.make_async_remote_copy(
        src_ref=src, dst_ref=dst, send_sem=ssem, recv_sem=rsem, device_id=to, device_id_type=MESH
    )


def ring_and_group(a, z, c):
    ids = [{"ctx": ctx_of(pa, z, pc)} for pa, pc in group_peers(a, c)]
    ids.append({"ctx": ctx_of(a, (z + 1) % RING, c)})
    ids.append({"ctx": ctx_of(a, (z + RING - 1) % RING, c)})
    return ids


def doc_starts(len_ref):
    starts = [jnp.int32(0)]
    for d in range(DOCS - 1):
        starts.append(starts[-1] + len_ref[0, d])
    return starts


def gather_kernel(len_ref, q_ref, do_ref, k_ref, v_ref,
                  qs, dog_ref, kg_ref, vg_ref, e_ref, top_ref, max_ref, sum_ref, ot,
                  kall, vall, qall, doall, begin_ref, gs, gr, xs, xr, rs, rr, ls):
    bf, f32 = jnp.bfloat16, jnp.float32
    a, z, c = place()
    ids = ring_and_group(a, z, c)
    own = 2 * a + c
    row0 = mult(a * HALF_SEQ + z * CHIP_ROWS + c * TOK, TOK)
    local = []
    for i, (src, dst) in enumerate(((k_ref, kall), (v_ref, vall))):
        local.append(pltpu.make_async_copy(
            src.at[:, pl.ds(mult(own * HEAD, HEAD), HEAD)], dst.at[pl.ds(row0, TOK)], ls.at[i]))
    wide = []
    for i, (src, dst) in enumerate(((q_ref, qall), (do_ref, doall))):
        wide.append(pltpu.make_async_copy(
            src.at[:, pl.ds(mult(own * 512, 512), 512)],
            dst.at[pl.ds(mult(own * TOK, TOK), TOK)], ls.at[2 + i]))
    for one in local + wide:
        one.start()
    enter(ids)
    sent = []
    peers = group_peers(a, c)
    for p, (pa, pc) in enumerate(peers):
        for i, (src, dst) in enumerate(((k_ref, kall), (v_ref, vall))):
            head = 2 * pa + pc
            cp = remote(src.at[:, pl.ds(mult(head * HEAD, HEAD), HEAD)], dst.at[pl.ds(row0, TOK)],
                        gs.at[2 * p + i], gr.at[2 * p + i], ids[p])
            cp.start()
            sent.append(cp)
    for i, (src, dst) in enumerate(((q_ref, qall), (do_ref, doall))):
        for p, (pa, pc) in enumerate(peers):
            head = 2 * pa + pc
            cp = remote(src.at[:, pl.ds(mult(head * 512, 512), 512)],
                        dst.at[pl.ds(mult(own * TOK, TOK), TOK)],
                        xs.at[2 * p + i], xr.at[2 * p + i], ids[p])
            cp.start()
            sent.append(cp)

    def group_arrived(p):
        pa, pc = peers[p]
        rows = pl.ds(mult(pa * HALF_SEQ + z * CHIP_ROWS + pc * TOK, TOK), TOK)
        for i, dst in enumerate((kall, vall)):
            remote(dst.at[rows], dst.at[rows], gs.at[2 * p + i], gr.at[2 * p + i], ids[p]).wait_recv()

    chunks = ((kall, a), (vall, a), (kall, 1 - a), (vall, 1 - a))
    ways = (1, -1)

    def chunk(j, zz):
        ref, y = chunks[j]
        return ref.at[pl.ds(mult(y * HALF_SEQ + zz * CHIP_ROWS, CHIP_ROWS), CHIP_ROWS)]

    def at(w, s, j):
        return (w * 4 + s) * 4 + j

    def send_on(w, s, j):
        part = chunk(j, (z + 2 * RING - ways[w] * s) % RING)
        cp = remote(part, part, rs.at[at(w, s, j)], rr.at[at(w, s, j)], ids[3 + w])
        cp.start()
        sent.append(cp)

    def arrived(w, s, j):
        part = chunk(j, (z + 2 * RING - ways[w] * (s + 1)) % RING)
        remote(part, part, rs.at[at(w, s, j)], rr.at[at(w, s, j)], ids[3 + w]).wait_recv()

    def carries(w, s, j):
        return s < 3 or (j < 2) == (w == 0)

    def position(t):
        return t * HALF_SEQ + z * CHIP_ROWS + lax.broadcasted_iota(jnp.int32, (1, WIDE), 1) % CHIP_ROWS

    def fold_in(t, y, zz, diagonal=False):
        first = y * HALF_SEQ + zz * CHIP_ROWS
        rows = pl.ds(mult(first, CHIP_ROWS), CHIP_ROWS)
        slot = t * RING + y * RING + zz
        key_pos = lax.broadcasted_iota(jnp.int32, (KB, WIDE), 0)
        visible = key_pos >= begin_ref[t] - first
        if diagonal:
            visible = visible & (key_pos <= position(t) - first)
        s = jnp.where(visible, nt(kall[rows, :], qs[t]), NEG)
        old = max_ref[t]
        new = jnp.maximum(old, jnp.max(s, axis=0, keepdims=True) * FOLD)
        e = jnp.exp2(s * FOLD - new)
        factor = jnp.exp2(old - new)
        sum_ref[t] = sum_ref[t] * factor + jnp.sum(e, axis=0, keepdims=True)
        eb = e.astype(bf)
        e_ref[slot] = eb
        top_ref[slot] = new
        max_ref[t] = new
        ot[t] = ot[t] * factor + nn(vall[rows, :].T, eb)

    def fold_both(y, s, w):
        zz = (z + 2 * RING - ways[w] * (s + 1)) % RING

        def one(t, carry):
            @pl.when(y * RING + zz <= t * RING + z)
            def _():
                fold_in(t, y, zz)

            return carry

        lax.fori_loop(0, 2, one, 0)

    def relay(s, half):
        for w in (0, 1):
            for j in (2 * half, 2 * half + 1):
                if carries(w, s, j):
                    arrived(w, s, j)
                    if s < 3 and carries(w, s + 1, j):
                        send_on(w, s + 1, j)
            if s > 0 and carries(w, s, 2 * half):
                fold_both(1 - a if half else a, s, w)

    for one in local:
        one.wait()
    group_arrived(0)
    for j in (0, 1):
        for w in (0, 1):
            send_on(w, 0, j)
    starts = doc_starts(len_ref)
    for t in range(2):
        begin = jnp.zeros((1, WIDE), jnp.int32)
        for at_start in starts:
            begin = jnp.where(at_start <= position(t), jnp.maximum(begin, at_start), begin)
        begin_ref[t] = begin
        max_ref[t] = jnp.full((1, WIDE), NEG, f32)
        sum_ref[t] = jnp.zeros((1, WIDE), f32)
        ot[t] = jnp.zeros((HEAD, WIDE), f32)
    group_arrived(1)
    group_arrived(2)
    for j in (2, 3):
        for w in (0, 1):
            send_on(w, 0, j)
    relay(0, 0)

    def crossed(i, dst):
        wide[i].wait()
        for p, (pa, pc) in enumerate(peers):
            rows = pl.ds(mult((2 * pa + pc) * TOK, TOK), TOK)
            remote(dst.at[rows], dst.at[rows], xs.at[2 * p + i], xr.at[2 * p + i], ids[p]).wait_recv()

    crossed(0, qall)
    for t in range(2):
        for h in range(GROUP):
            qs[t, h * CHIP_ROWS:(h + 1) * CHIP_ROWS, :] = qall[
                t * CHIP_ROWS:(t + 1) * CHIP_ROWS, h * HEAD:(h + 1) * HEAD]
    relay(0, 1)

    def own_tile(t, carry):
        fold_in(t, t, z, True)
        return carry

    lax.fori_loop(0, 2, own_tile, 0)
    fold_in(1, 0, z)
    for half in (0, 1):
        for w in (0, 1):
            fold_both(1 - a if half else a, 0, w)
        relay(1, half)
    for s in (2, 3):
        for half in (0, 1):
            relay(s, half)
    kg_ref[...] = kall[...]
    vg_ref[...] = vall[...]
    crossed(1, doall)
    dog_ref[...] = doall[...]
    for one in sent:
        one.wait_send()


def gather_call(lengths, q, do, k, v):
    bf, f32 = jnp.bfloat16, jnp.float32
    dma = pltpu.SemaphoreType.DMA
    return pl.pallas_call(
        gather_kernel,
        out_shape=(
            jax.ShapeDtypeStruct((2, WIDE, HEAD), bf), jax.ShapeDtypeStruct((512, 512), bf),
            jax.ShapeDtypeStruct((SEQ, HEAD), bf), jax.ShapeDtypeStruct((SEQ, HEAD), bf),
            jax.ShapeDtypeStruct((PAIRS, KB, WIDE), bf), jax.ShapeDtypeStruct((PAIRS, 1, WIDE), f32),
            jax.ShapeDtypeStruct((2, 1, WIDE), f32), jax.ShapeDtypeStruct((2, 1, WIDE), f32),
            jax.ShapeDtypeStruct((2, HEAD, WIDE), f32),
        ),
        in_specs=[SMEM] + [HBM] * 4,
        out_specs=(VMEM,) * 9,
        scratch_shapes=[
            pltpu.VMEM((SEQ, HEAD), bf), pltpu.VMEM((SEQ, HEAD), bf),
            pltpu.VMEM((512, 512), bf), pltpu.VMEM((512, 512), bf), pltpu.VMEM((2, 1, WIDE), jnp.int32),
            dma((6,)), dma((6,)), dma((6,)), dma((6,)), dma((32,)), dma((32,)), dma((4,)),
        ],
        compiler_params=pltpu.CompilerParams(
            collective_id=0, has_side_effects=True, vmem_limit_bytes=26 << 20),
        name="gather",
    )(lengths, q, do, k, v)


def attend_kernel(len_ref, q_ref, do_ref, k_ref, v_ref, e_ref, top_ref, max_ref, sum_ref, ot_ref,
                  dq_ref, dk_ref, dv_ref, kt, dos, dot_ref, dqt, dka, dva):
    _, z, _ = place()
    bf, f32 = jnp.bfloat16, jnp.float32

    def prepare(b, carry):
        kt[b] = k_ref[pl.ds(mult(b * KB, KB), KB), :].T
        dka[b] = jnp.zeros((KB, HEAD), f32)
        dva[b] = jnp.zeros((KB, HEAD), f32)
        return carry

    lax.fori_loop(0, NKB, prepare, 0)
    starts = doc_starts(len_ref)

    def tile(t, carry):
        first = t * HALF_SEQ + z * CHIP_ROWS
        rows = pl.ds(mult(t * CHIP_ROWS, CHIP_ROWS), CHIP_ROWS)
        for h in range(GROUP):
            part = slice(h * HEAD, (h + 1) * HEAD)
            stack = slice(h * CHIP_ROWS, (h + 1) * CHIP_ROWS)
            grads = do_ref[rows, part]
            dos[stack, :] = grads
            dot_ref[:, stack] = grads.astype(f32).T
        low = jnp.int32(0)
        for at in starts:
            low = jnp.where(at <= first, jnp.maximum(low, at), low)
        inverse = 1.0 / sum_ref[t]
        top = max_ref[t]
        delta = jnp.sum(dot_ref[...] * ot_ref[t], axis=0, keepdims=True) * inverse
        dqt[...] = jnp.zeros_like(dqt)

        def back(b, carry):
            slot = t * RING + b
            values = v_ref[pl.ds(mult(b * KB, KB), KB), :]
            factor = jnp.exp2(top_ref[slot] - top) * inverse
            p = e_ref[slot].astype(f32) * factor
            gp = nt(values, dos[...])
            ds = (p * (gp - delta)).astype(bf)
            dva[b] += nn(p.astype(bf), dos[...])
            dka[b] += nn(ds, q_ref[t])
            dqt[...] += nn(kt[b], ds)
            return carry

        lax.fori_loop(low // KB, first // KB + 1, back, 0)
        for h in range(GROUP):
            part = slice(h * HEAD, (h + 1) * HEAD)
            stack = slice(h * CHIP_ROWS, (h + 1) * CHIP_ROWS)
            dq_ref[rows, part] = (dqt[:, stack] * SCALE).T.astype(bf)
        return carry

    lax.fori_loop(0, 2, tile, 0)

    def finish(b, carry):
        rows = pl.ds(mult(b * KB, KB), KB)
        dk_ref[rows, :] = (dka[b] * SCALE).astype(bf)
        dv_ref[rows, :] = dva[b].astype(bf)
        return carry

    lax.fori_loop(0, NKB, finish, 0)


def attend_call(lengths, gathered):
    bf, f32 = jnp.bfloat16, jnp.float32
    return pl.pallas_call(
        attend_kernel,
        out_shape=(
            jax.ShapeDtypeStruct((512, 512), bf),
            jax.ShapeDtypeStruct((SEQ, HEAD), bf), jax.ShapeDtypeStruct((SEQ, HEAD), bf),
        ),
        in_specs=[SMEM] + [VMEM] * 9,
        out_specs=(VMEM,) * 3,
        scratch_shapes=[
            pltpu.VMEM((NKB, HEAD, KB), bf), pltpu.VMEM((WIDE, HEAD), bf),
            pltpu.VMEM((HEAD, WIDE), f32), pltpu.VMEM((HEAD, WIDE), f32),
            pltpu.VMEM((NKB, KB, HEAD), f32), pltpu.VMEM((NKB, KB, HEAD), f32),
        ],
        compiler_params=pltpu.CompilerParams(vmem_limit_bytes=20 << 20),
        name="attend",
    )(lengths, *gathered)


def reduce_kernel(dq_ref, dk_ref, dv_ref, hid_ref, qa_ref, qb_ref, va_ref, vb_ref,
                  dql_out, dkl_out, dvl_out, full_out,
                  rb, fin, dql, dkl, dvl, part, in1, h1, in2, h2, in3, full,
                  gs, gr, xs, xr, rs, rr, ls,
                  s1, r1, s2, r2, s3, r3, s4, r4, s5, r5):
    bf, f32 = jnp.bfloat16, jnp.float32
    a, z, c = place()
    ids = ring_and_group(a, z, c)
    own = 2 * a + c
    peers = group_peers(a, c)
    ways = (1, -1)
    chunks = ((dv_ref, 1 - a), (dv_ref, a), (dk_ref, 1 - a), (dk_ref, a))
    head_cols = pl.ds(mult(own * HEAD, HEAD), HEAD)
    wide_cols = pl.ds(mult(own * 512, 512), 512)
    seat = lax.axis_index("dp") * 2 + a
    sibling = ids[0]
    z_of = [(z + d) % RING for d in range(RING)]
    z_ids = [{"ctx": ctx_of(a, zz, c)} for zz in z_of]
    seats = [(seat + e) % 16 for e in range(16)]
    seat_ids = [{"dp": m // 2, "ctx": ctx_of(m % 2, z, c)} for m in seats]
    mine = pltpu.make_async_copy(
        dq_ref.at[pl.ds(mult(own * TOK, TOK), TOK)], dql.at[:, wide_cols], ls.at[0])
    mine.start()
    enter([sibling, ids[2]] + z_ids[1:] + seat_ids[1:])
    sent = []

    def go(src, dst, ssem, rsem, to):
        cp = remote(src, dst, ssem, rsem, to)
        cp.start()
        sent.append(cp)

    def came(dst, ssem, rsem, to):
        remote(dst, dst, ssem, rsem, to).wait_recv()

    def rows_of(j, dist):
        y = chunks[j][1]
        return pl.ds(mult(y * HALF_SEQ + ((z + 2 * RING + dist) % RING) * CHIP_ROWS, CHIP_ROWS), CHIP_ROWS)

    def at(w, d, j):
        return (w * 4 + d - 1) * 4 + j

    def starts_far(w, j):
        return (j % 2 == 0) == (w == 0)

    def send_on(w, d, j, src):
        k = at(w, d, j)
        go(src, rb.at[k], rs.at[k], rr.at[k], ids[3 + w])

    def arrived(w, d, j):
        k = at(w, d, j)
        came(rb.at[k], rs.at[k], rr.at[k], ids[3 + w])

    def half(which):
        return pl.ds(mult(which * CORE_COLS, CORE_COLS), CORE_COLS)

    def shard(zz):
        return pl.ds(mult(zz * Z_COLS, Z_COLS), Z_COLS)

    def core_send(u):
        go(part.at[u, :, half(1 - c)], in1.at[u], s1.at[u], r1.at[u], sibling)

    def z_send(u):
        came(in1.at[u], s1.at[u], r1.at[u], sibling)
        h1[u] = (part[u, :, half(c)].astype(f32) + in1[u].astype(f32)).astype(bf)
        for d in range(1, RING):
            k = u * 7 + d - 1
            go(h1.at[u, :, shard(z_of[d])], in2.at[k], s2.at[k], r2.at[k], z_ids[d])

    def seat_send(u):
        subtotal = h1[u, :, shard(z)].astype(f32)
        for d in range(1, RING):
            k = u * 7 + d - 1
            came(in2.at[k], s2.at[k], r2.at[k], z_ids[d])
            subtotal = subtotal + in2[k].astype(f32)
        h2[u] = subtotal.astype(bf)
        for e in range(1, 16):
            k = u * 15 + e - 1
            go(h2.at[u], in3.at[u, seat], s3.at[k], r3.at[k], seat_ids[e])
        in3[u, seat] = subtotal.astype(bf)

    def z_spread(u):
        for e in range(1, 16):
            k = u * 15 + e - 1
            came(in3.at[u, (seat + 16 - e) % 16], s3.at[k], r3.at[k], seat_ids[e])
        subtotal = in3[u, 0].astype(f32)
        for m in range(1, 16):
            subtotal = subtotal + in3[u, m].astype(f32)
        full[u, c, z] = subtotal.astype(bf)
        for d in range(1, RING):
            k = u * 7 + d - 1
            go(full.at[u, c, z], full.at[u, c, z], s4.at[k], r4.at[k], z_ids[d])

    def core_spread(u):
        for d in range(1, RING):
            k = u * 7 + d - 1
            came(full.at[u, c, (z + RING - d) % RING], s4.at[k], r4.at[k], z_ids[d])
        go(full.at[u, c], full.at[u, c], s5.at[u], r5.at[u], sibling)

    def collect(u):
        came(full.at[u, 1 - c], s5.at[u], r5.at[u], sibling)
        full_out[u] = full[u]

    def first_sends(js):
        for d, far in ((4, True), (3, False)):
            for j in js:
                for w in (0, 1):
                    if starts_far(w, j) == far:
                        send_on(w, d, j, chunks[j][0].at[rows_of(j, d * ways[w])])

    def forward(d, js):
        for j in js:
            for w in (0, 1):
                if d == 3 and not starts_far(w, j):
                    continue
                arrived(w, d + 1, j)
                slot = at(w, d + 1, j)
                own_part = chunks[j][0][rows_of(j, d * ways[w]), :].astype(f32)
                rb[slot] = (rb[slot].astype(f32) + own_part).astype(bf)
                send_on(w, d, j, rb.at[slot])

    def last(i, dst):
        for j in (2 * i, 2 * i + 1):
            for w in (0, 1):
                arrived(w, 1, j)
            both = rb[at(0, 1, j)].astype(f32) + rb[at(1, 1, j)].astype(f32)
            fin[j] = (both + chunks[j][0][rows_of(j, 0), :].astype(f32)).astype(bf)
            for p in ((1, 2) if j % 2 == 0 else (0,)):
                go(fin.at[j, pl.ds(mult(peers[p][1] * TOK, TOK), TOK)], dst.at[:, head_cols],
                   gs.at[2 * p + i], gr.at[2 * p + i], ids[p])
        one = pltpu.make_async_copy(
            fin.at[2 * i + 1, pl.ds(mult(c * TOK, TOK), TOK)], dst.at[:, head_cols], ls.at[1 + i])
        one.start()
        return one

    def returned(i, dst, own_copy):
        own_copy.wait()
        for p, (pa, pc) in enumerate(peers):
            cols = pl.ds(mult((2 * pa + pc) * HEAD, HEAD), HEAD)
            came(dst.at[:, cols], gs.at[2 * p + i], gr.at[2 * p + i], ids[p])

    values, keys = (0, 1), (2, 3)
    first_sends(values)
    for p, (pa, pc) in enumerate(peers):
        go(dq_ref.at[pl.ds(mult((2 * pa + pc) * TOK, TOK), TOK)], dql.at[:, wide_cols],
           xs.at[p], xr.at[p], ids[p])
    hidden = hid_ref[...]
    query_proj = nt(qa_ref[...], hidden).astype(bf)
    value_proj = nt(va_ref[...], hidden).astype(bf)
    part[1, :, 4608:PACKED] = jnp.zeros((RANK, PACKED - 4608), bf)
    forward(3, values)
    forward(2, values)
    forward(1, values)
    first_sends(keys)
    own_values = last(0, dvl)
    mine.wait()
    for p, (pa, pc) in enumerate(peers):
        cols = pl.ds(mult((2 * pa + pc) * 512, 512), 512)
        came(dql.at[:, cols], xs.at[p], xr.at[p], ids[p])
    query = dql[...]
    part[0, :, 4096:6144] = (2.0 * nn(query_proj, query)).astype(bf)
    query_low = nt(qb_ref[...], query).astype(bf)
    part[0, :, 0:4096] = (2.0 * nn(query_low, hidden)).astype(bf)
    core_send(0)
    forward(3, keys)
    returned(0, dvl, own_values)
    value = dvl[...]
    part[1, :, 4096:4608] = (2.0 * nn(value_proj, value)).astype(bf)
    value_low = nt(vb_ref[...], value).astype(bf)
    part[1, :, 0:4096] = (2.0 * nn(value_low, hidden)).astype(bf)
    core_send(1)
    z_send(0)
    z_send(1)
    forward(2, keys)
    seat_send(0)
    seat_send(1)
    forward(1, keys)
    dql_out[...] = query
    dvl_out[...] = value
    z_spread(0)
    own_keys = last(1, dkl)
    z_spread(1)
    core_spread(0)
    returned(1, dkl, own_keys)
    dkl_out[...] = dkl[...]
    core_spread(1)
    collect(0)
    collect(1)
    for one in sent:
        one.wait_send()


def reduce_call(dq, dk, dv, hidden, qa, qb, va, vb):
    bf = jnp.bfloat16
    dma = pltpu.SemaphoreType.DMA
    return pl.pallas_call(
        reduce_kernel,
        out_shape=(
            jax.ShapeDtypeStruct((TOK, 2048), bf), jax.ShapeDtypeStruct((TOK, 512), bf),
            jax.ShapeDtypeStruct((TOK, 512), bf),
            jax.ShapeDtypeStruct((2, 2, RING, RANK, Z_COLS), bf),
        ),
        in_specs=[VMEM] * 8,
        out_specs=(VMEM,) * 4,
        scratch_shapes=[
            pltpu.VMEM((32, CHIP_ROWS, HEAD), bf), pltpu.VMEM((4, CHIP_ROWS, HEAD), bf),
            pltpu.VMEM((TOK, 2048), bf), pltpu.VMEM((TOK, 512), bf), pltpu.VMEM((TOK, 512), bf),
            pltpu.VMEM((2, RANK, PACKED), bf), pltpu.VMEM((2, RANK, CORE_COLS), bf),
            pltpu.VMEM((2, RANK, CORE_COLS), bf), pltpu.VMEM((14, RANK, Z_COLS), bf),
            pltpu.VMEM((2, RANK, Z_COLS), bf), pltpu.VMEM((2, 16, RANK, Z_COLS), bf),
            pltpu.VMEM((2, 2, RING, RANK, Z_COLS), bf),
            dma((6,)), dma((6,)), dma((3,)), dma((3,)), dma((32,)), dma((32,)), dma((3,)),
            dma((2,)), dma((2,)), dma((14,)), dma((14,)), dma((30,)), dma((30,)),
            dma((14,)), dma((14,)), dma((2,)), dma((2,)),
        ],
        compiler_params=pltpu.CompilerParams(
            collective_id=1, has_side_effects=True, vmem_limit_bytes=24 << 20),
        name="reduce",
    )(dq, dk, dv, hidden, qa, qb, va, vb)


SPANS = ((0, 0, 4096), (0, 4096, 6144), (1, 0, 4096), (1, 4096, 4608))


def finish_kernel(dql_ref, dkl_ref, dvl_ref, full_ref, dq_out, dk_out, dv_out,
                  qa_out, qb_out, va_out, vb_out, sem):
    copies = []
    for i, (src, dst) in enumerate(((dql_ref, dq_out), (dkl_ref, dk_out), (dvl_ref, dv_out))):
        copies.append(pltpu.make_async_copy(src, dst, sem.at[i]))
    for one in copies:
        one.start()
    for out, (u, begin, end) in zip((qa_out, qb_out, va_out, vb_out), SPANS):
        for cc in range(2):
            for zz in range(RING):
                lo = cc * CORE_COLS + zz * Z_COLS
                x, y = max(lo, begin), min(lo + Z_COLS, end)
                if x < y:
                    out[:, x - begin:y - begin] = full_ref[u, cc, zz, :, x - lo:y - lo].astype(jnp.float32)
    for one in copies:
        one.wait()


def finish_call(dql, dkl, dvl, full):
    bf = jnp.bfloat16
    return pl.pallas_call(
        finish_kernel,
        out_shape=(
            jax.ShapeDtypeStruct((TOK, 2048), bf), jax.ShapeDtypeStruct((TOK, 512), bf),
            jax.ShapeDtypeStruct((TOK, 512), bf),
        ) + tuple(jax.ShapeDtypeStruct((RANK, e - b), jnp.float32) for _, b, e in SPANS),
        in_specs=[VMEM] * 4,
        out_specs=(ANY,) * 3 + (VMEM,) * 4,
        scratch_shapes=[pltpu.SemaphoreType.DMA((3,))],
        compiler_params=pltpu.CompilerParams(vmem_limit_bytes=8 << 20),
        name="finish",
    )(dql, dkl, dvl, full)


def shards(q, k, v, do, hidden, lengths, qa, qb, va, vb):
    gathered = gather_call(lengths, q[0], do[0], k[0], v[0])
    dq, dk, dv = attend_call(lengths, gathered)
    landed = reduce_call(dq, dk, dv, hidden[0], qa, qb, va, vb)
    out = finish_call(*landed)
    return (out[0][None], out[1][None], out[2][None]) + tuple(out[3:])


def solution(mesh):
    token = P("dp", "ctx", None)
    return jax.shard_map(
        shards,
        mesh=mesh,
        in_specs=(token, token, token, token, token, P("dp", None), P(), P(), P(), P()),
        out_specs=(token, token, token, P(), P(), P(), P()),
        check_vma=False,
    )
```

```python
import math

import jax
import jax.numpy as jnp
from jax import lax
from jax.experimental import pallas as pl
from jax.experimental.pallas import tpu as pltpu
from jax.sharding import PartitionSpec as P

MESH = pl.DeviceIdType.MESH
HEAD = 128
GROUP = 4
TOK = 128
RING = 8
CHIP_ROWS = 256
HALF_SEQ = 2048
SEQ = 4096
KB = 256
WIDE = GROUP * CHIP_ROWS
PAIRS = SEQ // KB + HALF_SEQ // KB
FOLD = HEAD ** (-0.5) * math.log2(math.e)
NKB = SEQ // KB
RANK = 16
PACKED = 6144
CORE_COLS = PACKED // 2
Z_COLS = CORE_COLS // RING
DOCS = 16
NEG = -1e30
SCALE = HEAD ** (-0.5)
ANY = pl.BlockSpec(memory_space=pl.ANY)
VMEM = pl.BlockSpec(memory_space=pltpu.VMEM)
SMEM = pl.BlockSpec(memory_space=pltpu.SMEM)
HBM = pl.BlockSpec(memory_space=pltpu.HBM)


def nn(left, right):
    return lax.dot_general(left, right, (((1,), (0,)), ((), ())), preferred_element_type=jnp.float32)


def nt(left, right):
    return lax.dot_general(left, right, (((1,), (1,)), ((), ())), preferred_element_type=jnp.float32)


def place():
    me = lax.axis_index("ctx")
    return me // 16, (me // 2) % RING, me % 2


def ctx_of(a, z, c):
    return a * 16 + z * 2 + c


def mult(value, of):
    return pl.multiple_of(value, of)


def group_peers(a, c):
    return ((a, 1 - c), (1 - a, c), (1 - a, 1 - c))


def enter(ids):
    barrier = pltpu.get_barrier_semaphore()
    for one in ids:
        pl.semaphore_signal(barrier, inc=1, device_id=one, device_id_type=MESH)
    pl.semaphore_wait(barrier, len(ids))


def remote(src, dst, ssem, rsem, to):
    return pltpu.make_async_remote_copy(
        src_ref=src, dst_ref=dst, send_sem=ssem, recv_sem=rsem, device_id=to, device_id_type=MESH
    )


def ring_and_group(a, z, c):
    ids = [{"ctx": ctx_of(pa, z, pc)} for pa, pc in group_peers(a, c)]
    ids.append({"ctx": ctx_of(a, (z + 1) % RING, c)})
    ids.append({"ctx": ctx_of(a, (z + RING - 1) % RING, c)})
    return ids


def doc_starts(len_ref):
    starts = [jnp.int32(0)]
    for d in range(DOCS - 1):
        starts.append(starts[-1] + len_ref[0, d])
    return starts


def gather_kernel(len_ref, q_ref, do_ref, k_ref, v_ref,
                  qs, dog_ref, kg_ref, vg_ref, e_ref, top_ref, max_ref, sum_ref, ot,
                  kall, vall, qall, doall, begin_ref, gs, gr, xs, xr, rs, rr, ls):
    bf, f32 = jnp.bfloat16, jnp.float32
    a, z, c = place()
    ids = ring_and_group(a, z, c)
    own = 2 * a + c
    row0 = mult(a * HALF_SEQ + z * CHIP_ROWS + c * TOK, TOK)
    local = []
    for i, (src, dst) in enumerate(((k_ref, kall), (v_ref, vall))):
        local.append(pltpu.make_async_copy(
            src.at[:, pl.ds(mult(own * HEAD, HEAD), HEAD)], dst.at[pl.ds(row0, TOK)], ls.at[i]))
    wide = []
    for i, (src, dst) in enumerate(((q_ref, qall), (do_ref, doall))):
        wide.append(pltpu.make_async_copy(
            src.at[:, pl.ds(mult(own * 512, 512), 512)],
            dst.at[pl.ds(mult(own * TOK, TOK), TOK)], ls.at[2 + i]))
    for one in local + wide:
        one.start()
    enter(ids)
    sent = []
    peers = group_peers(a, c)
    for p, (pa, pc) in enumerate(peers):
        for i, (src, dst) in enumerate(((k_ref, kall), (v_ref, vall))):
            head = 2 * pa + pc
            cp = remote(src.at[:, pl.ds(mult(head * HEAD, HEAD), HEAD)], dst.at[pl.ds(row0, TOK)],
                        gs.at[2 * p + i], gr.at[2 * p + i], ids[p])
            cp.start()
            sent.append(cp)
    for i, (src, dst) in enumerate(((q_ref, qall), (do_ref, doall))):
        for p, (pa, pc) in enumerate(peers):
            head = 2 * pa + pc
            cp = remote(src.at[:, pl.ds(mult(head * 512, 512), 512)],
                        dst.at[pl.ds(mult(own * TOK, TOK), TOK)],
                        xs.at[2 * p + i], xr.at[2 * p + i], ids[p])
            cp.start()
            sent.append(cp)

    def group_arrived(p):
        pa, pc = peers[p]
        rows = pl.ds(mult(pa * HALF_SEQ + z * CHIP_ROWS + pc * TOK, TOK), TOK)
        for i, dst in enumerate((kall, vall)):
            remote(dst.at[rows], dst.at[rows], gs.at[2 * p + i], gr.at[2 * p + i], ids[p]).wait_recv()

    chunks = ((kall, a), (vall, a), (kall, 1 - a), (vall, 1 - a))
    ways = (1, -1)

    def chunk(j, zz):
        ref, y = chunks[j]
        return ref.at[pl.ds(mult(y * HALF_SEQ + zz * CHIP_ROWS, CHIP_ROWS), CHIP_ROWS)]

    def at(w, s, j):
        return (w * 4 + s) * 4 + j

    def send_on(w, s, j):
        part = chunk(j, (z + 2 * RING - ways[w] * s) % RING)
        cp = remote(part, part, rs.at[at(w, s, j)], rr.at[at(w, s, j)], ids[3 + w])
        cp.start()
        sent.append(cp)

    def arrived(w, s, j):
        part = chunk(j, (z + 2 * RING - ways[w] * (s + 1)) % RING)
        remote(part, part, rs.at[at(w, s, j)], rr.at[at(w, s, j)], ids[3 + w]).wait_recv()

    def carries(w, s, j):
        return s < 3 or (j < 2) == (w == 0)

    def position(t):
        return t * HALF_SEQ + z * CHIP_ROWS + lax.broadcasted_iota(jnp.int32, (1, WIDE), 1) % CHIP_ROWS

    def fold_in(t, y, zz, diagonal=False):
        first = y * HALF_SEQ + zz * CHIP_ROWS
        rows = pl.ds(mult(first, CHIP_ROWS), CHIP_ROWS)
        slot = t * RING + y * RING + zz
        key_pos = lax.broadcasted_iota(jnp.int32, (KB, WIDE), 0)
        visible = key_pos >= begin_ref[t] - first
        if diagonal:
            visible = visible & (key_pos <= position(t) - first)
        s = jnp.where(visible, nt(kall[rows, :], qs[t]), NEG)
        old = max_ref[t]
        new = jnp.maximum(old, jnp.max(s, axis=0, keepdims=True) * FOLD)
        e = jnp.exp2(s * FOLD - new)
        factor = jnp.exp2(old - new)
        sum_ref[t] = sum_ref[t] * factor + jnp.sum(e, axis=0, keepdims=True)
        eb = e.astype(bf)
        e_ref[slot] = eb
        top_ref[slot] = new
        max_ref[t] = new
        ot[t] = ot[t] * factor + nn(vall[rows, :].T, eb)

    def fold_both(y, s, w):
        zz = (z + 2 * RING - ways[w] * (s + 1)) % RING

        def one(t, carry):
            @pl.when(y * RING + zz <= t * RING + z)
            def _():
                fold_in(t, y, zz)

            return carry

        lax.fori_loop(0, 2, one, 0)

    def relay(s, half):
        for w in (0, 1):
            for j in (2 * half, 2 * half + 1):
                if carries(w, s, j):
                    arrived(w, s, j)
                    if s < 3 and carries(w, s + 1, j):
                        send_on(w, s + 1, j)
            if s > 0 and carries(w, s, 2 * half):
                fold_both(1 - a if half else a, s, w)

    for one in local:
        one.wait()
    group_arrived(0)
    for j in (0, 1):
        for w in (0, 1):
            send_on(w, 0, j)
    starts = doc_starts(len_ref)
    for t in range(2):
        begin = jnp.zeros((1, WIDE), jnp.int32)
        for at_start in starts:
            begin = jnp.where(at_start <= position(t), jnp.maximum(begin, at_start), begin)
        begin_ref[t] = begin
        max_ref[t] = jnp.full((1, WIDE), NEG, f32)
        sum_ref[t] = jnp.zeros((1, WIDE), f32)
        ot[t] = jnp.zeros((HEAD, WIDE), f32)
    group_arrived(1)
    group_arrived(2)
    for j in (2, 3):
        for w in (0, 1):
            send_on(w, 0, j)
    relay(0, 0)

    def crossed(i, dst):
        wide[i].wait()
        for p, (pa, pc) in enumerate(peers):
            rows = pl.ds(mult((2 * pa + pc) * TOK, TOK), TOK)
            remote(dst.at[rows], dst.at[rows], xs.at[2 * p + i], xr.at[2 * p + i], ids[p]).wait_recv()

    crossed(0, qall)
    for t in range(2):
        for h in range(GROUP):
            qs[t, h * CHIP_ROWS:(h + 1) * CHIP_ROWS, :] = qall[
                t * CHIP_ROWS:(t + 1) * CHIP_ROWS, h * HEAD:(h + 1) * HEAD]
    relay(0, 1)

    def own_tile(t, carry):
        fold_in(t, t, z, True)
        return carry

    lax.fori_loop(0, 2, own_tile, 0)
    fold_in(1, 0, z)
    for half in (0, 1):
        for w in (0, 1):
            fold_both(1 - a if half else a, 0, w)
        relay(1, half)
    for s in (2, 3):
        for half in (0, 1):
            relay(s, half)
    kg_ref[...] = kall[...]
    vg_ref[...] = vall[...]
    crossed(1, doall)
    dog_ref[...] = doall[...]
    for one in sent:
        one.wait_send()


def gather_call(lengths, q, do, k, v):
    bf, f32 = jnp.bfloat16, jnp.float32
    dma = pltpu.SemaphoreType.DMA
    return pl.pallas_call(
        gather_kernel,
        out_shape=(
            jax.ShapeDtypeStruct((2, WIDE, HEAD), bf), jax.ShapeDtypeStruct((512, 512), bf),
            jax.ShapeDtypeStruct((SEQ, HEAD), bf), jax.ShapeDtypeStruct((SEQ, HEAD), bf),
            jax.ShapeDtypeStruct((PAIRS, KB, WIDE), bf), jax.ShapeDtypeStruct((PAIRS, 1, WIDE), f32),
            jax.ShapeDtypeStruct((2, 1, WIDE), f32), jax.ShapeDtypeStruct((2, 1, WIDE), f32),
            jax.ShapeDtypeStruct((2, HEAD, WIDE), f32),
        ),
        in_specs=[SMEM] + [HBM] * 4,
        out_specs=(VMEM,) * 9,
        scratch_shapes=[
            pltpu.VMEM((SEQ, HEAD), bf), pltpu.VMEM((SEQ, HEAD), bf),
            pltpu.VMEM((512, 512), bf), pltpu.VMEM((512, 512), bf), pltpu.VMEM((2, 1, WIDE), jnp.int32),
            dma((6,)), dma((6,)), dma((6,)), dma((6,)), dma((32,)), dma((32,)), dma((4,)),
        ],
        compiler_params=pltpu.CompilerParams(
            collective_id=0, has_side_effects=True, vmem_limit_bytes=26 << 20),
        name="gather",
    )(lengths, q, do, k, v)


def attend_kernel(len_ref, q_ref, do_ref, k_ref, v_ref, e_ref, top_ref, max_ref, sum_ref, ot_ref,
                  dq_ref, dk_ref, dv_ref, kt, dos, dot_ref, dqt, dka, dva):
    _, z, _ = place()
    bf, f32 = jnp.bfloat16, jnp.float32

    def prepare(b, carry):
        kt[b] = k_ref[pl.ds(mult(b * KB, KB), KB), :].T
        dka[b] = jnp.zeros((KB, HEAD), f32)
        dva[b] = jnp.zeros((KB, HEAD), f32)
        return carry

    lax.fori_loop(0, NKB, prepare, 0)
    starts = doc_starts(len_ref)

    def tile(t, carry):
        first = t * HALF_SEQ + z * CHIP_ROWS
        rows = pl.ds(mult(t * CHIP_ROWS, CHIP_ROWS), CHIP_ROWS)
        for h in range(GROUP):
            part = slice(h * HEAD, (h + 1) * HEAD)
            stack = slice(h * CHIP_ROWS, (h + 1) * CHIP_ROWS)
            grads = do_ref[rows, part]
            dos[stack, :] = grads
            dot_ref[:, stack] = grads.astype(f32).T
        low = jnp.int32(0)
        for at in starts:
            low = jnp.where(at <= first, jnp.maximum(low, at), low)
        inverse = 1.0 / sum_ref[t]
        top = max_ref[t]
        delta = jnp.sum(dot_ref[...] * ot_ref[t], axis=0, keepdims=True) * inverse
        dqt[...] = jnp.zeros_like(dqt)

        def back(b, carry):
            slot = t * RING + b
            values = v_ref[pl.ds(mult(b * KB, KB), KB), :]
            factor = jnp.exp2(top_ref[slot] - top) * inverse
            p = e_ref[slot].astype(f32) * factor
            gp = nt(values, dos[...])
            ds = (p * (gp - delta)).astype(bf)
            dva[b] += nn(p.astype(bf), dos[...])
            dka[b] += nn(ds, q_ref[t])
            dqt[...] += nn(kt[b], ds)
            return carry

        lax.fori_loop(low // KB, first // KB + 1, back, 0)
        for h in range(GROUP):
            part = slice(h * HEAD, (h + 1) * HEAD)
            stack = slice(h * CHIP_ROWS, (h + 1) * CHIP_ROWS)
            dq_ref[rows, part] = (dqt[:, stack] * SCALE).T.astype(bf)
        return carry

    lax.fori_loop(0, 2, tile, 0)

    def finish(b, carry):
        rows = pl.ds(mult(b * KB, KB), KB)
        dk_ref[rows, :] = (dka[b] * SCALE).astype(bf)
        dv_ref[rows, :] = dva[b].astype(bf)
        return carry

    lax.fori_loop(0, NKB, finish, 0)


def attend_call(lengths, gathered):
    bf, f32 = jnp.bfloat16, jnp.float32
    return pl.pallas_call(
        attend_kernel,
        out_shape=(
            jax.ShapeDtypeStruct((512, 512), bf),
            jax.ShapeDtypeStruct((SEQ, HEAD), bf), jax.ShapeDtypeStruct((SEQ, HEAD), bf),
        ),
        in_specs=[SMEM] + [VMEM] * 9,
        out_specs=(VMEM,) * 3,
        scratch_shapes=[
            pltpu.VMEM((NKB, HEAD, KB), bf), pltpu.VMEM((WIDE, HEAD), bf),
            pltpu.VMEM((HEAD, WIDE), f32), pltpu.VMEM((HEAD, WIDE), f32),
            pltpu.VMEM((NKB, KB, HEAD), f32), pltpu.VMEM((NKB, KB, HEAD), f32),
        ],
        compiler_params=pltpu.CompilerParams(vmem_limit_bytes=20 << 20),
        name="attend",
    )(lengths, *gathered)


def reduce_kernel(dq_ref, dk_ref, dv_ref, hid_ref, qa_ref, qb_ref, va_ref, vb_ref,
                  dql_out, dkl_out, dvl_out, full_out,
                  rb, fin, dql, dkl, dvl, part, in1, h1, in2, h2, in3, full,
                  gs, gr, xs, xr, rs, rr, ls,
                  s1, r1, s2, r2, s3, r3, s4, r4, s5, r5):
    bf, f32 = jnp.bfloat16, jnp.float32
    a, z, c = place()
    ids = ring_and_group(a, z, c)
    own = 2 * a + c
    peers = group_peers(a, c)
    ways = (1, -1)
    spots = ((1 - a, c), (1 - a, 1 - c), (a, 1 - c), (a, c))
    chunks = tuple((ref, y, side) for ref in (dv_ref, dk_ref) for y, side in spots)
    head_cols = pl.ds(mult(own * HEAD, HEAD), HEAD)
    wide_cols = pl.ds(mult(own * 512, 512), 512)
    seat = lax.axis_index("dp") * 2 + a
    sibling = ids[0]
    z_of = [(z + d) % RING for d in range(RING)]
    z_ids = [{"ctx": ctx_of(a, zz, c)} for zz in z_of]
    seats = [(seat + e) % 16 for e in range(16)]
    seat_ids = [{"dp": m // 2, "ctx": ctx_of(m % 2, z, c)} for m in seats]
    mine = pltpu.make_async_copy(
        dq_ref.at[pl.ds(mult(own * TOK, TOK), TOK)], dql.at[:, wide_cols], ls.at[0])
    mine.start()
    enter([sibling, ids[2]] + z_ids[1:] + seat_ids[1:])
    sent = []

    def go(src, dst, ssem, rsem, to):
        cp = remote(src, dst, ssem, rsem, to)
        cp.start()
        sent.append(cp)

    def came(dst, ssem, rsem, to):
        remote(dst, dst, ssem, rsem, to).wait_recv()

    def rows_of(j, dist):
        _, y, side = chunks[j]
        return pl.ds(mult(y * HALF_SEQ + ((z + 2 * RING + dist) % RING) * CHIP_ROWS + side * TOK, TOK), TOK)

    def at(w, d, j):
        return (w * 4 + d - 1) * 8 + j

    def starts_far(w, j):
        return (j % 2 == 0) == (w == 0)

    def send_on(w, d, j, src):
        k = at(w, d, j)
        go(src, rb.at[k], rs.at[k], rr.at[k], ids[3 + w])

    def arrived(w, d, j):
        k = at(w, d, j)
        came(rb.at[k], rs.at[k], rr.at[k], ids[3 + w])

    def half(which):
        return pl.ds(mult(which * CORE_COLS, CORE_COLS), CORE_COLS)

    def shard(zz):
        return pl.ds(mult(zz * Z_COLS, Z_COLS), Z_COLS)

    def core_send(u):
        go(part.at[u, :, half(1 - c)], in1.at[u], s1.at[u], r1.at[u], sibling)

    def z_send(u):
        came(in1.at[u], s1.at[u], r1.at[u], sibling)
        h1[u] = (part[u, :, half(c)].astype(f32) + in1[u].astype(f32)).astype(bf)
        for d in range(1, RING):
            k = u * 7 + d - 1
            go(h1.at[u, :, shard(z_of[d])], in2.at[k], s2.at[k], r2.at[k], z_ids[d])

    def seat_send(u):
        subtotal = h1[u, :, shard(z)].astype(f32)
        for d in range(1, RING):
            k = u * 7 + d - 1
            came(in2.at[k], s2.at[k], r2.at[k], z_ids[d])
            subtotal = subtotal + in2[k].astype(f32)
        h2[u] = subtotal.astype(bf)
        for e in range(1, 16):
            k = u * 15 + e - 1
            go(h2.at[u], in3.at[u, seat], s3.at[k], r3.at[k], seat_ids[e])
        in3[u, seat] = subtotal.astype(bf)

    def z_spread(u):
        for e in range(1, 16):
            k = u * 15 + e - 1
            came(in3.at[u, (seat + 16 - e) % 16], s3.at[k], r3.at[k], seat_ids[e])
        subtotal = in3[u, 0].astype(f32)
        for m in range(1, 16):
            subtotal = subtotal + in3[u, m].astype(f32)
        full[u, c, z] = subtotal.astype(bf)
        for d in range(1, RING):
            k = u * 7 + d - 1
            go(full.at[u, c, z], full.at[u, c, z], s4.at[k], r4.at[k], z_ids[d])

    def core_spread(u):
        for d in range(1, RING):
            k = u * 7 + d - 1
            came(full.at[u, c, (z + RING - d) % RING], s4.at[k], r4.at[k], z_ids[d])
        go(full.at[u, c], full.at[u, c], s5.at[u], r5.at[u], sibling)

    def collect(u):
        came(full.at[u, 1 - c], s5.at[u], r5.at[u], sibling)
        full_out[u] = full[u]

    def first_sends(js):
        for d, far in ((4, True), (3, False)):
            for j in js:
                for w in (0, 1):
                    if starts_far(w, j) == far:
                        send_on(w, d, j, chunks[j][0].at[rows_of(j, d * ways[w])])

    def forward(d, js):
        for j in js:
            for w in (0, 1):
                if d == 3 and not starts_far(w, j):
                    continue
                arrived(w, d + 1, j)
                slot = at(w, d + 1, j)
                own_part = chunks[j][0][rows_of(j, d * ways[w]), :].astype(f32)
                rb[slot] = (rb[slot].astype(f32) + own_part).astype(bf)
                send_on(w, d, j, rb.at[slot])

    def last(i, dst):
        for k, p in enumerate((1, 2, 0, None)):
            j = 4 * i + k
            for w in (0, 1):
                arrived(w, 1, j)
            both = rb[at(0, 1, j)].astype(f32) + rb[at(1, 1, j)].astype(f32)
            fin[j] = (both + chunks[j][0][rows_of(j, 0), :].astype(f32)).astype(bf)
            if p is not None:
                go(fin.at[j], dst.at[:, head_cols], gs.at[2 * p + i], gr.at[2 * p + i], ids[p])
        one = pltpu.make_async_copy(fin.at[4 * i + 3], dst.at[:, head_cols], ls.at[1 + i])
        one.start()
        return one

    def returned(i, dst, own_copy):
        own_copy.wait()
        for p, (pa, pc) in enumerate(peers):
            cols = pl.ds(mult((2 * pa + pc) * HEAD, HEAD), HEAD)
            came(dst.at[:, cols], gs.at[2 * p + i], gr.at[2 * p + i], ids[p])

    values, keys = (0, 1, 2, 3), (4, 5, 6, 7)
    first_sends(values)
    for p, (pa, pc) in enumerate(peers):
        go(dq_ref.at[pl.ds(mult((2 * pa + pc) * TOK, TOK), TOK)], dql.at[:, wide_cols],
           xs.at[p], xr.at[p], ids[p])
    hidden = hid_ref[...]
    query_proj = nt(qa_ref[...], hidden).astype(bf)
    value_proj = nt(va_ref[...], hidden).astype(bf)
    part[1, :, 4608:PACKED] = jnp.zeros((RANK, PACKED - 4608), bf)
    forward(3, values)
    forward(2, values)
    forward(1, values)
    first_sends(keys)
    own_values = last(0, dvl)
    mine.wait()
    for p, (pa, pc) in enumerate(peers):
        cols = pl.ds(mult((2 * pa + pc) * 512, 512), 512)
        came(dql.at[:, cols], xs.at[p], xr.at[p], ids[p])
    query = dql[...]
    part[0, :, 4096:6144] = (2.0 * nn(query_proj, query)).astype(bf)
    query_low = nt(qb_ref[...], query).astype(bf)
    part[0, :, 0:4096] = (2.0 * nn(query_low, hidden)).astype(bf)
    core_send(0)
    forward(3, keys)
    returned(0, dvl, own_values)
    value = dvl[...]
    part[1, :, 4096:4608] = (2.0 * nn(value_proj, value)).astype(bf)
    value_low = nt(vb_ref[...], value).astype(bf)
    part[1, :, 0:4096] = (2.0 * nn(value_low, hidden)).astype(bf)
    core_send(1)
    z_send(0)
    z_send(1)
    forward(2, keys)
    seat_send(0)
    seat_send(1)
    forward(1, keys)
    dql_out[...] = query
    dvl_out[...] = value
    z_spread(0)
    own_keys = last(1, dkl)
    z_spread(1)
    core_spread(0)
    returned(1, dkl, own_keys)
    dkl_out[...] = dkl[...]
    core_spread(1)
    collect(0)
    collect(1)
    for one in sent:
        one.wait_send()


def reduce_call(dq, dk, dv, hidden, qa, qb, va, vb):
    bf = jnp.bfloat16
    dma = pltpu.SemaphoreType.DMA
    return pl.pallas_call(
        reduce_kernel,
        out_shape=(
            jax.ShapeDtypeStruct((TOK, 2048), bf), jax.ShapeDtypeStruct((TOK, 512), bf),
            jax.ShapeDtypeStruct((TOK, 512), bf),
            jax.ShapeDtypeStruct((2, 2, RING, RANK, Z_COLS), bf),
        ),
        in_specs=[VMEM] * 8,
        out_specs=(VMEM,) * 4,
        scratch_shapes=[
            pltpu.VMEM((64, TOK, HEAD), bf), pltpu.VMEM((8, TOK, HEAD), bf),
            pltpu.VMEM((TOK, 2048), bf), pltpu.VMEM((TOK, 512), bf), pltpu.VMEM((TOK, 512), bf),
            pltpu.VMEM((2, RANK, PACKED), bf), pltpu.VMEM((2, RANK, CORE_COLS), bf),
            pltpu.VMEM((2, RANK, CORE_COLS), bf), pltpu.VMEM((14, RANK, Z_COLS), bf),
            pltpu.VMEM((2, RANK, Z_COLS), bf), pltpu.VMEM((2, 16, RANK, Z_COLS), bf),
            pltpu.VMEM((2, 2, RING, RANK, Z_COLS), bf),
            dma((6,)), dma((6,)), dma((3,)), dma((3,)), dma((64,)), dma((64,)), dma((3,)),
            dma((2,)), dma((2,)), dma((14,)), dma((14,)), dma((30,)), dma((30,)),
            dma((14,)), dma((14,)), dma((2,)), dma((2,)),
        ],
        compiler_params=pltpu.CompilerParams(
            collective_id=1, has_side_effects=True, vmem_limit_bytes=24 << 20),
        name="reduce",
    )(dq, dk, dv, hidden, qa, qb, va, vb)


SPANS = ((0, 0, 4096), (0, 4096, 6144), (1, 0, 4096), (1, 4096, 4608))


def finish_kernel(dql_ref, dkl_ref, dvl_ref, full_ref, dq_out, dk_out, dv_out,
                  qa_out, qb_out, va_out, vb_out, sem):
    copies = []
    for i, (src, dst) in enumerate(((dql_ref, dq_out), (dkl_ref, dk_out), (dvl_ref, dv_out))):
        copies.append(pltpu.make_async_copy(src, dst, sem.at[i]))
    for one in copies:
        one.start()
    for out, (u, begin, end) in zip((qa_out, qb_out, va_out, vb_out), SPANS):
        for cc in range(2):
            for zz in range(RING):
                lo = cc * CORE_COLS + zz * Z_COLS
                x, y = max(lo, begin), min(lo + Z_COLS, end)
                if x < y:
                    out[:, x - begin:y - begin] = full_ref[u, cc, zz, :, x - lo:y - lo].astype(jnp.float32)
    for one in copies:
        one.wait()


def finish_call(dql, dkl, dvl, full):
    bf = jnp.bfloat16
    return pl.pallas_call(
        finish_kernel,
        out_shape=(
            jax.ShapeDtypeStruct((TOK, 2048), bf), jax.ShapeDtypeStruct((TOK, 512), bf),
            jax.ShapeDtypeStruct((TOK, 512), bf),
        ) + tuple(jax.ShapeDtypeStruct((RANK, e - b), jnp.float32) for _, b, e in SPANS),
        in_specs=[VMEM] * 4,
        out_specs=(ANY,) * 3 + (VMEM,) * 4,
        scratch_shapes=[pltpu.SemaphoreType.DMA((3,))],
        compiler_params=pltpu.CompilerParams(vmem_limit_bytes=8 << 20),
        name="finish",
    )(dql, dkl, dvl, full)


def shards(q, k, v, do, hidden, lengths, qa, qb, va, vb):
    gathered = gather_call(lengths, q[0], do[0], k[0], v[0])
    dq, dk, dv = attend_call(lengths, gathered)
    landed = reduce_call(dq, dk, dv, hidden[0], qa, qb, va, vb)
    out = finish_call(*landed)
    return (out[0][None], out[1][None], out[2][None]) + tuple(out[3:])


def solution(mesh):
    token = P("dp", "ctx", None)
    return jax.shard_map(
        shards,
        mesh=mesh,
        in_specs=(token, token, token, token, token, P("dp", None), P(), P(), P(), P()),
        out_specs=(token, token, token, P(), P(), P(), P()),
        check_vma=False,
    )
```

```python
import math

import jax
import jax.numpy as jnp
from jax import lax
from jax.experimental import pallas as pl
from jax.experimental.pallas import tpu as pltpu
from jax.sharding import PartitionSpec as P

MESH = pl.DeviceIdType.MESH
HEAD = 128
GROUP = 4
TOK = 128
RING = 8
CHIP_ROWS = 256
HALF_SEQ = 2048
SEQ = 4096
KB = 256
WIDE = GROUP * CHIP_ROWS
PAIRS = SEQ // KB + HALF_SEQ // KB
FOLD = HEAD ** (-0.5) * math.log2(math.e)
NKB = SEQ // KB
RANK = 16
PACKED = 6144
CORE_COLS = PACKED // 2
Z_COLS = CORE_COLS // RING
DOCS = 16
NEG = -1e30
SCALE = HEAD ** (-0.5)
ANY = pl.BlockSpec(memory_space=pl.ANY)
VMEM = pl.BlockSpec(memory_space=pltpu.VMEM)
SMEM = pl.BlockSpec(memory_space=pltpu.SMEM)
HBM = pl.BlockSpec(memory_space=pltpu.HBM)


def nn(left, right):
    return lax.dot_general(left, right, (((1,), (0,)), ((), ())), preferred_element_type=jnp.float32)


def nt(left, right):
    return lax.dot_general(left, right, (((1,), (1,)), ((), ())), preferred_element_type=jnp.float32)


def place():
    me = lax.axis_index("ctx")
    return me // 16, (me // 2) % RING, me % 2


def ctx_of(a, z, c):
    return a * 16 + z * 2 + c


def mult(value, of):
    return pl.multiple_of(value, of)


def group_peers(a, c):
    return ((a, 1 - c), (1 - a, c), (1 - a, 1 - c))


def enter(ids):
    barrier = pltpu.get_barrier_semaphore()
    for one in ids:
        pl.semaphore_signal(barrier, inc=1, device_id=one, device_id_type=MESH)
    pl.semaphore_wait(barrier, len(ids))


def remote(src, dst, ssem, rsem, to):
    return pltpu.make_async_remote_copy(
        src_ref=src, dst_ref=dst, send_sem=ssem, recv_sem=rsem, device_id=to, device_id_type=MESH
    )


def ring_and_group(a, z, c):
    ids = [{"ctx": ctx_of(pa, z, pc)} for pa, pc in group_peers(a, c)]
    ids.append({"ctx": ctx_of(a, (z + 1) % RING, c)})
    ids.append({"ctx": ctx_of(a, (z + RING - 1) % RING, c)})
    return ids


def doc_starts(len_ref):
    starts = [jnp.int32(0)]
    for d in range(DOCS - 1):
        starts.append(starts[-1] + len_ref[0, d])
    return starts


def gather_kernel(len_ref, q_ref, do_ref, k_ref, v_ref,
                  qs, dog_ref, kg_ref, vg_ref, e_ref, top_ref, max_ref, sum_ref, ot,
                  kall, vall, qall, doall, begin_ref, gs, gr, xs, xr, rs, rr, ls):
    bf, f32 = jnp.bfloat16, jnp.float32
    a, z, c = place()
    ids = ring_and_group(a, z, c)
    own = 2 * a + c
    row0 = mult(a * HALF_SEQ + z * CHIP_ROWS + c * TOK, TOK)
    local = []
    for i, (src, dst) in enumerate(((k_ref, kall), (v_ref, vall))):
        local.append(pltpu.make_async_copy(
            src.at[:, pl.ds(mult(own * HEAD, HEAD), HEAD)], dst.at[pl.ds(row0, TOK)], ls.at[i]))
    wide = []
    for i, (src, dst) in enumerate(((q_ref, qall), (do_ref, doall))):
        wide.append(pltpu.make_async_copy(
            src.at[:, pl.ds(mult(own * 512, 512), 512)],
            dst.at[pl.ds(mult(own * TOK, TOK), TOK)], ls.at[2 + i]))
    for one in local + wide:
        one.start()
    enter(ids)
    sent = []
    peers = group_peers(a, c)
    for p, (pa, pc) in enumerate(peers):
        for i, (src, dst) in enumerate(((k_ref, kall), (v_ref, vall))):
            head = 2 * pa + pc
            cp = remote(src.at[:, pl.ds(mult(head * HEAD, HEAD), HEAD)], dst.at[pl.ds(row0, TOK)],
                        gs.at[2 * p + i], gr.at[2 * p + i], ids[p])
            cp.start()
            sent.append(cp)
    for i, (src, dst) in enumerate(((q_ref, qall), (do_ref, doall))):
        for p, (pa, pc) in enumerate(peers):
            head = 2 * pa + pc
            cp = remote(src.at[:, pl.ds(mult(head * 512, 512), 512)],
                        dst.at[pl.ds(mult(own * TOK, TOK), TOK)],
                        xs.at[2 * p + i], xr.at[2 * p + i], ids[p])
            cp.start()
            sent.append(cp)

    def group_arrived(p):
        pa, pc = peers[p]
        rows = pl.ds(mult(pa * HALF_SEQ + z * CHIP_ROWS + pc * TOK, TOK), TOK)
        for i, dst in enumerate((kall, vall)):
            remote(dst.at[rows], dst.at[rows], gs.at[2 * p + i], gr.at[2 * p + i], ids[p]).wait_recv()

    chunks = ((kall, a), (vall, a), (kall, 1 - a), (vall, 1 - a))
    ways = (1, -1)

    def chunk(j, zz):
        ref, y = chunks[j]
        return ref.at[pl.ds(mult(y * HALF_SEQ + zz * CHIP_ROWS, CHIP_ROWS), CHIP_ROWS)]

    def at(w, s, j):
        return (w * 4 + s) * 4 + j

    def send_on(w, s, j):
        part = chunk(j, (z + 2 * RING - ways[w] * s) % RING)
        cp = remote(part, part, rs.at[at(w, s, j)], rr.at[at(w, s, j)], ids[3 + w])
        cp.start()
        sent.append(cp)

    def arrived(w, s, j):
        part = chunk(j, (z + 2 * RING - ways[w] * (s + 1)) % RING)
        remote(part, part, rs.at[at(w, s, j)], rr.at[at(w, s, j)], ids[3 + w]).wait_recv()

    def carries(w, s, j):
        return s < 3 or (j < 2) == (w == 0)

    def position(t):
        return t * HALF_SEQ + z * CHIP_ROWS + lax.broadcasted_iota(jnp.int32, (1, WIDE), 1) % CHIP_ROWS

    def fold_in(t, y, zz, diagonal=False):
        first = y * HALF_SEQ + zz * CHIP_ROWS
        rows = pl.ds(mult(first, CHIP_ROWS), CHIP_ROWS)
        slot = t * RING + y * RING + zz
        key_pos = lax.broadcasted_iota(jnp.int32, (KB, WIDE), 0)
        visible = key_pos >= begin_ref[t] - first
        if diagonal:
            visible = visible & (key_pos <= position(t) - first)
        s = jnp.where(visible, nt(kall[rows, :], qs[t]), NEG)
        old = max_ref[t]
        new = jnp.maximum(old, jnp.max(s, axis=0, keepdims=True) * FOLD)
        e = jnp.exp2(s * FOLD - new)
        factor = jnp.exp2(old - new)
        sum_ref[t] = sum_ref[t] * factor + jnp.sum(e, axis=0, keepdims=True)
        eb = e.astype(bf)
        e_ref[slot] = eb
        top_ref[slot] = new
        max_ref[t] = new
        ot[t] = ot[t] * factor + nn(vall[rows, :].T, eb)

    def fold_both(y, s, w):
        zz = (z + 2 * RING - ways[w] * (s + 1)) % RING

        def one(t, carry):
            @pl.when(y * RING + zz <= t * RING + z)
            def _():
                fold_in(t, y, zz)

            return carry

        lax.fori_loop(0, 2, one, 0)

    def relay(s, half):
        for w in (0, 1):
            for j in (2 * half, 2 * half + 1):
                if carries(w, s, j):
                    arrived(w, s, j)
                    if s < 3 and carries(w, s + 1, j):
                        send_on(w, s + 1, j)
            if s > 0 and carries(w, s, 2 * half):
                fold_both(1 - a if half else a, s, w)

    for one in local:
        one.wait()
    group_arrived(0)
    for j in (0, 1):
        for w in (0, 1):
            send_on(w, 0, j)
    starts = doc_starts(len_ref)
    for t in range(2):
        begin = jnp.zeros((1, WIDE), jnp.int32)
        for at_start in starts:
            begin = jnp.where(at_start <= position(t), jnp.maximum(begin, at_start), begin)
        begin_ref[t] = begin
        max_ref[t] = jnp.full((1, WIDE), NEG, f32)
        sum_ref[t] = jnp.zeros((1, WIDE), f32)
        ot[t] = jnp.zeros((HEAD, WIDE), f32)
    group_arrived(1)
    group_arrived(2)
    for j in (2, 3):
        for w in (0, 1):
            send_on(w, 0, j)
    relay(0, 0)

    def crossed(i, dst):
        wide[i].wait()
        for p, (pa, pc) in enumerate(peers):
            rows = pl.ds(mult((2 * pa + pc) * TOK, TOK), TOK)
            remote(dst.at[rows], dst.at[rows], xs.at[2 * p + i], xr.at[2 * p + i], ids[p]).wait_recv()

    crossed(0, qall)
    for t in range(2):
        for h in range(GROUP):
            qs[t, h * CHIP_ROWS:(h + 1) * CHIP_ROWS, :] = qall[
                t * CHIP_ROWS:(t + 1) * CHIP_ROWS, h * HEAD:(h + 1) * HEAD]
    relay(0, 1)

    def own_tile(t, carry):
        fold_in(t, t, z, True)
        return carry

    lax.fori_loop(0, 2, own_tile, 0)
    fold_in(1, 0, z)
    for half in (0, 1):
        for w in (0, 1):
            fold_both(1 - a if half else a, 0, w)
        relay(1, half)
    for half in (0, 1):
        relay(2, half)
    crossed(1, doall)
    dog_ref[...] = doall[...]
    for half in (0, 1):
        relay(3, half)
    kg_ref[...] = kall[...]
    vg_ref[...] = vall[...]
    for one in sent:
        one.wait_send()


def gather_call(lengths, q, do, k, v):
    bf, f32 = jnp.bfloat16, jnp.float32
    dma = pltpu.SemaphoreType.DMA
    return pl.pallas_call(
        gather_kernel,
        out_shape=(
            jax.ShapeDtypeStruct((2, WIDE, HEAD), bf), jax.ShapeDtypeStruct((512, 512), bf),
            jax.ShapeDtypeStruct((SEQ, HEAD), bf), jax.ShapeDtypeStruct((SEQ, HEAD), bf),
            jax.ShapeDtypeStruct((PAIRS, KB, WIDE), bf), jax.ShapeDtypeStruct((PAIRS, 1, WIDE), f32),
            jax.ShapeDtypeStruct((2, 1, WIDE), f32), jax.ShapeDtypeStruct((2, 1, WIDE), f32),
            jax.ShapeDtypeStruct((2, HEAD, WIDE), f32),
        ),
        in_specs=[SMEM] + [HBM] * 4,
        out_specs=(VMEM,) * 9,
        scratch_shapes=[
            pltpu.VMEM((SEQ, HEAD), bf), pltpu.VMEM((SEQ, HEAD), bf),
            pltpu.VMEM((512, 512), bf), pltpu.VMEM((512, 512), bf), pltpu.VMEM((2, 1, WIDE), jnp.int32),
            dma((6,)), dma((6,)), dma((6,)), dma((6,)), dma((32,)), dma((32,)), dma((4,)),
        ],
        compiler_params=pltpu.CompilerParams(
            collective_id=0, has_side_effects=True, vmem_limit_bytes=26 << 20),
        name="gather",
    )(lengths, q, do, k, v)


def attend_kernel(len_ref, q_ref, do_ref, k_ref, v_ref, e_ref, top_ref, max_ref, sum_ref, ot_ref,
                  dq_ref, dk_ref, dv_ref, kt, dos, dot_ref, dqt, dka, dva):
    _, z, _ = place()
    bf, f32 = jnp.bfloat16, jnp.float32

    def prepare(b, carry):
        kt[b] = k_ref[pl.ds(mult(b * KB, KB), KB), :].T
        dka[b] = jnp.zeros((KB, HEAD), f32)
        dva[b] = jnp.zeros((KB, HEAD), f32)
        return carry

    lax.fori_loop(0, NKB, prepare, 0)
    starts = doc_starts(len_ref)

    def tile(t, carry):
        first = t * HALF_SEQ + z * CHIP_ROWS
        rows = pl.ds(mult(t * CHIP_ROWS, CHIP_ROWS), CHIP_ROWS)
        for h in range(GROUP):
            part = slice(h * HEAD, (h + 1) * HEAD)
            stack = slice(h * CHIP_ROWS, (h + 1) * CHIP_ROWS)
            grads = do_ref[rows, part]
            dos[stack, :] = grads
            dot_ref[:, stack] = grads.astype(f32).T
        low = jnp.int32(0)
        for at in starts:
            low = jnp.where(at <= first, jnp.maximum(low, at), low)
        inverse = 1.0 / sum_ref[t]
        top = max_ref[t]
        delta = jnp.sum(dot_ref[...] * ot_ref[t], axis=0, keepdims=True) * inverse
        dqt[...] = jnp.zeros_like(dqt)

        def back(b, carry):
            slot = t * RING + b
            values = v_ref[pl.ds(mult(b * KB, KB), KB), :]
            factor = jnp.exp2(top_ref[slot] - top) * inverse
            p = e_ref[slot].astype(f32) * factor
            gp = nt(values, dos[...])
            ds = (p * (gp - delta)).astype(bf)
            dva[b] += nn(p.astype(bf), dos[...])
            dka[b] += nn(ds, q_ref[t])
            dqt[...] += nn(kt[b], ds)
            return carry

        lax.fori_loop(low // KB, first // KB + 1, back, 0)
        for h in range(GROUP):
            part = slice(h * HEAD, (h + 1) * HEAD)
            stack = slice(h * CHIP_ROWS, (h + 1) * CHIP_ROWS)
            dq_ref[rows, part] = (dqt[:, stack] * SCALE).T.astype(bf)
        return carry

    lax.fori_loop(0, 2, tile, 0)

    def finish(b, carry):
        rows = pl.ds(mult(b * KB, KB), KB)
        dk_ref[rows, :] = (dka[b] * SCALE).astype(bf)
        dv_ref[rows, :] = dva[b].astype(bf)
        return carry

    lax.fori_loop(0, NKB, finish, 0)


def attend_call(lengths, gathered):
    bf, f32 = jnp.bfloat16, jnp.float32
    return pl.pallas_call(
        attend_kernel,
        out_shape=(
            jax.ShapeDtypeStruct((512, 512), bf),
            jax.ShapeDtypeStruct((SEQ, HEAD), bf), jax.ShapeDtypeStruct((SEQ, HEAD), bf),
        ),
        in_specs=[SMEM] + [VMEM] * 9,
        out_specs=(VMEM,) * 3,
        scratch_shapes=[
            pltpu.VMEM((NKB, HEAD, KB), bf), pltpu.VMEM((WIDE, HEAD), bf),
            pltpu.VMEM((HEAD, WIDE), f32), pltpu.VMEM((HEAD, WIDE), f32),
            pltpu.VMEM((NKB, KB, HEAD), f32), pltpu.VMEM((NKB, KB, HEAD), f32),
        ],
        compiler_params=pltpu.CompilerParams(vmem_limit_bytes=20 << 20),
        name="attend",
    )(lengths, *gathered)


def reduce_kernel(dq_ref, dk_ref, dv_ref, hid_ref, qa_ref, qb_ref, va_ref, vb_ref,
                  dql_out, dkl_out, dvl_out, full_out,
                  rb, fin, dql, dkl, dvl, part, in1, h1, in2, h2, in3, full,
                  gs, gr, xs, xr, rs, rr, ls,
                  s1, r1, s2, r2, s3, r3, s4, r4, s5, r5):
    bf, f32 = jnp.bfloat16, jnp.float32
    a, z, c = place()
    ids = ring_and_group(a, z, c)
    own = 2 * a + c
    peers = group_peers(a, c)
    ways = (1, -1)
    spots = ((1 - a, c), (1 - a, 1 - c), (a, 1 - c), (a, c))
    chunks = tuple((ref, y, side) for ref in (dv_ref, dk_ref) for y, side in spots)
    head_cols = pl.ds(mult(own * HEAD, HEAD), HEAD)
    wide_cols = pl.ds(mult(own * 512, 512), 512)
    seat = lax.axis_index("dp") * 2 + a
    sibling = ids[0]
    z_of = [(z + d) % RING for d in range(RING)]
    z_ids = [{"ctx": ctx_of(a, zz, c)} for zz in z_of]
    seats = [(seat + e) % 16 for e in range(16)]
    seat_ids = [{"dp": m // 2, "ctx": ctx_of(m % 2, z, c)} for m in seats]
    mine = pltpu.make_async_copy(
        dq_ref.at[pl.ds(mult(own * TOK, TOK), TOK)], dql.at[:, wide_cols], ls.at[0])
    mine.start()
    enter([sibling, ids[2]] + z_ids[1:] + seat_ids[1:])
    sent = []

    def go(src, dst, ssem, rsem, to):
        cp = remote(src, dst, ssem, rsem, to)
        cp.start()
        sent.append(cp)

    def came(dst, ssem, rsem, to):
        remote(dst, dst, ssem, rsem, to).wait_recv()

    def rows_of(j, dist):
        _, y, side = chunks[j]
        return pl.ds(mult(y * HALF_SEQ + ((z + 2 * RING + dist) % RING) * CHIP_ROWS + side * TOK, TOK), TOK)

    def at(w, d, j):
        return (w * 4 + d - 1) * 8 + j

    def starts_far(w, j):
        return (j % 2 == 0) == (w == 0)

    def send_on(w, d, j, src):
        k = at(w, d, j)
        go(src, rb.at[k], rs.at[k], rr.at[k], ids[3 + w])

    def arrived(w, d, j):
        k = at(w, d, j)
        came(rb.at[k], rs.at[k], rr.at[k], ids[3 + w])

    def half(which):
        return pl.ds(mult(which * CORE_COLS, CORE_COLS), CORE_COLS)

    def shard(zz):
        return pl.ds(mult(zz * Z_COLS, Z_COLS), Z_COLS)

    def core_send(u):
        go(part.at[u, :, half(1 - c)], in1.at[u], s1.at[u], r1.at[u], sibling)

    def z_send(u):
        came(in1.at[u], s1.at[u], r1.at[u], sibling)
        h1[u] = (part[u, :, half(c)].astype(f32) + in1[u].astype(f32)).astype(bf)
        for d in range(1, RING):
            k = u * 7 + d - 1
            go(h1.at[u, :, shard(z_of[d])], in2.at[k], s2.at[k], r2.at[k], z_ids[d])

    def seat_send(u):
        subtotal = h1[u, :, shard(z)].astype(f32)
        for d in range(1, RING):
            k = u * 7 + d - 1
            came(in2.at[k], s2.at[k], r2.at[k], z_ids[d])
            subtotal = subtotal + in2[k].astype(f32)
        h2[u] = subtotal.astype(bf)
        for e in range(1, 16):
            k = u * 15 + e - 1
            go(h2.at[u], in3.at[u, seat], s3.at[k], r3.at[k], seat_ids[e])
        in3[u, seat] = subtotal.astype(bf)

    def z_spread(u):
        for e in range(1, 16):
            k = u * 15 + e - 1
            came(in3.at[u, (seat + 16 - e) % 16], s3.at[k], r3.at[k], seat_ids[e])
        subtotal = in3[u, 0].astype(f32)
        for m in range(1, 16):
            subtotal = subtotal + in3[u, m].astype(f32)
        full[u, c, z] = subtotal.astype(bf)
        for d in range(1, RING):
            k = u * 7 + d - 1
            go(full.at[u, c, z], full.at[u, c, z], s4.at[k], r4.at[k], z_ids[d])

    def core_spread(u):
        for d in range(1, RING):
            k = u * 7 + d - 1
            came(full.at[u, c, (z + RING - d) % RING], s4.at[k], r4.at[k], z_ids[d])
        go(full.at[u, c], full.at[u, c], s5.at[u], r5.at[u], sibling)

    def collect(u):
        came(full.at[u, 1 - c], s5.at[u], r5.at[u], sibling)
        full_out[u] = full[u]

    def first_sends(js):
        for d, far in ((4, True), (3, False)):
            for j in js:
                for w in (0, 1):
                    if starts_far(w, j) == far:
                        send_on(w, d, j, chunks[j][0].at[rows_of(j, d * ways[w])])

    def forward(d, js):
        for j in js:
            for w in (0, 1):
                if d == 3 and not starts_far(w, j):
                    continue
                arrived(w, d + 1, j)
                slot = at(w, d + 1, j)
                own_part = chunks[j][0][rows_of(j, d * ways[w]), :].astype(f32)
                rb[slot] = (rb[slot].astype(f32) + own_part).astype(bf)
                send_on(w, d, j, rb.at[slot])

    def last(i, dst):
        for k, p in enumerate((1, 2, 0, None)):
            j = 4 * i + k
            for w in (0, 1):
                arrived(w, 1, j)
            both = rb[at(0, 1, j)].astype(f32) + rb[at(1, 1, j)].astype(f32)
            fin[j] = (both + chunks[j][0][rows_of(j, 0), :].astype(f32)).astype(bf)
            if p is not None:
                go(fin.at[j], dst.at[:, head_cols], gs.at[2 * p + i], gr.at[2 * p + i], ids[p])
        one = pltpu.make_async_copy(fin.at[4 * i + 3], dst.at[:, head_cols], ls.at[1 + i])
        one.start()
        return one

    def returned(i, dst, own_copy):
        own_copy.wait()
        for p, (pa, pc) in enumerate(peers):
            cols = pl.ds(mult((2 * pa + pc) * HEAD, HEAD), HEAD)
            came(dst.at[:, cols], gs.at[2 * p + i], gr.at[2 * p + i], ids[p])

    values, keys = (0, 1, 2, 3), (4, 5, 6, 7)
    first_sends(values)
    for p, (pa, pc) in enumerate(peers):
        go(dq_ref.at[pl.ds(mult((2 * pa + pc) * TOK, TOK), TOK)], dql.at[:, wide_cols],
           xs.at[p], xr.at[p], ids[p])
    hidden = hid_ref[...]
    query_proj = nt(qa_ref[...], hidden).astype(bf)
    value_proj = nt(va_ref[...], hidden).astype(bf)
    part[1, :, 4608:PACKED] = jnp.zeros((RANK, PACKED - 4608), bf)
    forward(3, values)
    forward(2, values)
    forward(1, values)
    first_sends(keys)
    own_values = last(0, dvl)
    mine.wait()
    for p, (pa, pc) in enumerate(peers):
        cols = pl.ds(mult((2 * pa + pc) * 512, 512), 512)
        came(dql.at[:, cols], xs.at[p], xr.at[p], ids[p])
    query = dql[...]
    part[0, :, 4096:6144] = (2.0 * nn(query_proj, query)).astype(bf)
    query_low = nt(qb_ref[...], query).astype(bf)
    part[0, :, 0:4096] = (2.0 * nn(query_low, hidden)).astype(bf)
    core_send(0)
    forward(3, keys)
    z_send(0)
    returned(0, dvl, own_values)
    value = dvl[...]
    part[1, :, 4096:4608] = (2.0 * nn(value_proj, value)).astype(bf)
    value_low = nt(vb_ref[...], value).astype(bf)
    part[1, :, 0:4096] = (2.0 * nn(value_low, hidden)).astype(bf)
    core_send(1)
    z_send(1)
    forward(2, keys)
    seat_send(0)
    seat_send(1)
    forward(1, keys)
    dql_out[...] = query
    dvl_out[...] = value
    z_spread(0)
    own_keys = last(1, dkl)
    z_spread(1)
    core_spread(0)
    returned(1, dkl, own_keys)
    dkl_out[...] = dkl[...]
    core_spread(1)
    collect(0)
    collect(1)
    for one in sent:
        one.wait_send()


def reduce_call(dq, dk, dv, hidden, qa, qb, va, vb):
    bf = jnp.bfloat16
    dma = pltpu.SemaphoreType.DMA
    return pl.pallas_call(
        reduce_kernel,
        out_shape=(
            jax.ShapeDtypeStruct((TOK, 2048), bf), jax.ShapeDtypeStruct((TOK, 512), bf),
            jax.ShapeDtypeStruct((TOK, 512), bf),
            jax.ShapeDtypeStruct((2, 2, RING, RANK, Z_COLS), bf),
        ),
        in_specs=[VMEM] * 8,
        out_specs=(VMEM,) * 4,
        scratch_shapes=[
            pltpu.VMEM((64, TOK, HEAD), bf), pltpu.VMEM((8, TOK, HEAD), bf),
            pltpu.VMEM((TOK, 2048), bf), pltpu.VMEM((TOK, 512), bf), pltpu.VMEM((TOK, 512), bf),
            pltpu.VMEM((2, RANK, PACKED), bf), pltpu.VMEM((2, RANK, CORE_COLS), bf),
            pltpu.VMEM((2, RANK, CORE_COLS), bf), pltpu.VMEM((14, RANK, Z_COLS), bf),
            pltpu.VMEM((2, RANK, Z_COLS), bf), pltpu.VMEM((2, 16, RANK, Z_COLS), bf),
            pltpu.VMEM((2, 2, RING, RANK, Z_COLS), bf),
            dma((6,)), dma((6,)), dma((3,)), dma((3,)), dma((64,)), dma((64,)), dma((3,)),
            dma((2,)), dma((2,)), dma((14,)), dma((14,)), dma((30,)), dma((30,)),
            dma((14,)), dma((14,)), dma((2,)), dma((2,)),
        ],
        compiler_params=pltpu.CompilerParams(
            collective_id=1, has_side_effects=True, vmem_limit_bytes=24 << 20),
        name="reduce",
    )(dq, dk, dv, hidden, qa, qb, va, vb)


SPANS = ((0, 0, 4096), (0, 4096, 6144), (1, 0, 4096), (1, 4096, 4608))


def finish_kernel(dql_ref, dkl_ref, dvl_ref, full_ref, dq_out, dk_out, dv_out,
                  qa_out, qb_out, va_out, vb_out, sem):
    copies = []
    for i, (src, dst) in enumerate(((dql_ref, dq_out), (dkl_ref, dk_out), (dvl_ref, dv_out))):
        copies.append(pltpu.make_async_copy(src, dst, sem.at[i]))
    for one in copies:
        one.start()
    for out, (u, begin, end) in zip((qa_out, qb_out, va_out, vb_out), SPANS):
        for cc in range(2):
            for zz in range(RING):
                lo = cc * CORE_COLS + zz * Z_COLS
                x, y = max(lo, begin), min(lo + Z_COLS, end)
                if x < y:
                    out[:, x - begin:y - begin] = full_ref[u, cc, zz, :, x - lo:y - lo].astype(jnp.float32)
    for one in copies:
        one.wait()


def finish_call(dql, dkl, dvl, full):
    bf = jnp.bfloat16
    return pl.pallas_call(
        finish_kernel,
        out_shape=(
            jax.ShapeDtypeStruct((TOK, 2048), bf), jax.ShapeDtypeStruct((TOK, 512), bf),
            jax.ShapeDtypeStruct((TOK, 512), bf),
        ) + tuple(jax.ShapeDtypeStruct((RANK, e - b), jnp.float32) for _, b, e in SPANS),
        in_specs=[VMEM] * 4,
        out_specs=(ANY,) * 3 + (VMEM,) * 4,
        scratch_shapes=[pltpu.SemaphoreType.DMA((3,))],
        compiler_params=pltpu.CompilerParams(vmem_limit_bytes=8 << 20),
        name="finish",
    )(dql, dkl, dvl, full)


def shards(q, k, v, do, hidden, lengths, qa, qb, va, vb):
    gathered = gather_call(lengths, q[0], do[0], k[0], v[0])
    dq, dk, dv = attend_call(lengths, gathered)
    landed = reduce_call(dq, dk, dv, hidden[0], qa, qb, va, vb)
    out = finish_call(*landed)
    return (out[0][None], out[1][None], out[2][None]) + tuple(out[3:])


def solution(mesh):
    token = P("dp", "ctx", None)
    return jax.shard_map(
        shards,
        mesh=mesh,
        in_specs=(token, token, token, token, token, P("dp", None), P(), P(), P(), P()),
        out_specs=(token, token, token, P(), P(), P(), P()),
        check_vma=False,
    )
```
